32 devices in a mesh: loader: 8 (over z, x), split: 4 (over y, core).
Axes of the slice: x: 2, y: 2, z: 4, core: 2. Of those that a mesh axis runs over, the one named last changes fastest.
Arguments:
- embeddings: bfloat16 [16384, 768], P(('loader', 'split')), may hold values from -6 to 6
- cluster_ids: int32 [16384, 1], P(('loader', 'split')), may hold values from 0 to 255; in each aligned block of 512 rows (0 to 511, 512 to 1023, ...) at most 4 rows name the same one
- ranks: int32 [16384], P(('loader', 'split')), may hold values from 0 to 16383, each once
Outputs:
- nearest: float32 [16384], P(('loader', 'split'))
The draws below stay inside these ranges and needn't reach their ends.
Inputs may be any that keep to these rules, and one draw needn't show every extreme that they name: `cluster_ids`: among the 512 rows of one device no cluster appears more than 4 times. All ranks differ.
All inputs are finite; a program needn't handle non-finite values.
Results may differ from the reference program's by a relative error of at most 0.0014.
Values may be sent and summed in bfloat16 or wider, within the bound.
A program may use at most 64 MiB of HBM per device.

```python
import math
import jax
import jax.numpy as jnp
import numpy as np
from jax import lax

D = 768
ROWS_DEV = 512
CLUSTERS = 256
CAP = 4
ROWS = 16384
WINDOW = 128


def steps_of(stream_key, extent, cuts, least, largest):
    factor_of, own = 1.0, jax.random.fold_in(stream_key, 6)
    for dim, parts in cuts:
        steps = jnp.exp(jax.random.uniform(jax.random.fold_in(own, dim), (parts,), jnp.float32, least / len(cuts), largest / len(cuts)))
        factor_of = factor_of * jnp.repeat(steps, extent[dim] // parts).reshape([-1 if axis == dim else 1 for axis in range(len(extent))])
    return factor_of


def routed_block(stream_key, own, number, rows, count, top, limit, skew):
    order = jax.random.permutation(stream_key, count)
    crowded, common = load_shares(count, rows * top, limit, skew, True), load_shares(count, rows * top, limit, skew, False)
    places = jnp.arange(count)

    def named(lengths, turn):
        used = int((lengths > 0).sum())
        fixed = max(1, used // 4)
        shifted = fixed + (places - fixed + turn * (used - fixed)) % max(1, count - fixed)
        return jnp.zeros((count,), jnp.int32).at[order[jnp.where(places < fixed, places, shifted)]].set(jnp.asarray(lengths, jnp.int32))

    lengths = jnp.where(number % 4 == 0, named(crowded, number // 4), named(common, number - number // 4 - 1))
    mixed = jax.random.permutation(jax.random.fold_in(own, 3), count)
    giver, taker = mixed[0:count // 2 * 2:2], mixed[1:count // 2 * 2:2]
    margin = jnp.minimum(lengths[giver] - 1, limit - lengths[taker]) // 2
    margin = jnp.where((giver == order[0]) | (taker == order[0]) | (lengths[taker] == 0), 0, jnp.maximum(margin, 0))
    shifted = jax.random.randint(jax.random.fold_in(own, 4), (count // 2,), 0, 1 << 20) % (margin + 1)
    lengths = lengths.at[giver].add(-shifted).at[taker].add(shifted)
    items = jnp.searchsorted(jnp.cumsum(lengths), jnp.arange(rows * top), side="right").astype(jnp.int32)
    grid = items.reshape(top, rows).T
    grid = grid[jax.random.permutation(jax.random.fold_in(own, 1), rows)]
    turn = jax.random.randint(jax.random.fold_in(own, 2), (rows, 1), 0, top)
    return jnp.take_along_axis(grid, (jnp.arange(top)[None, :] + turn) % top, axis=1)


def load_shares(amount, total, most, lean, full):
    portions = [(1 << 20) // math.isqrt(standing ** lean) + 1 for standing in range(1, amount + 1)]
    largest = most if full else min(most, max(-(-total // amount), total * portions[0] // sum(portions)))
    least = 1 if total - largest >= amount - 1 else 0
    given, surplus = [largest] + [least] * (amount - 1), total - largest - least * (amount - 1)
    while surplus > 0:
        movable = [i for i in range(1, amount) if given[i] < largest] or [i for i in range(1, amount) if given[i] < most]
        whole, left = sum([portions[i] for i in movable]), surplus
        for i in movable:
            addition = min(most - given[i], max(1, left * portions[i] // whole), surplus)
            given[i] = given[i] + addition
            surplus = surplus - addition
    return np.array(given)


def scatter_about(own_key, dims, scale, limit, cuts=(), kind=jnp.bfloat16):
    entries = jax.random.normal(own_key, dims, jnp.float32) * scale
    if len(cuts) > 0:
        entries = steps_of(own_key, dims, cuts, -0.22, 0.18) * entries
    return jnp.clip(entries, min=-limit, max=limit).astype(kind)


def setup_inputs(seed: int = 0) -> dict:
    keys = jax.random.split(jax.random.key(seed), 4)
    embeddings = scatter_about(keys[0], (ROWS, D), 1.0, 6.0, ((0, 32),))
    cluster_ids_keys = jax.random.split(jax.random.fold_in(keys[1], 1), ROWS // ROWS_DEV)
    cluster_ids_turns = jax.random.permutation(jax.random.fold_in(keys[1], 3), ROWS // ROWS_DEV)
    cluster_ids = jax.vmap(lambda own, number: routed_block(jax.random.fold_in(keys[1], 2), own, number, ROWS_DEV, CLUSTERS, 1, CAP, 2))(cluster_ids_keys, cluster_ids_turns).reshape((ROWS, 1))
    ranks = jax.random.permutation(keys[2], ROWS).astype(jnp.int32)
    return dict(embeddings=embeddings, cluster_ids=cluster_ids, ranks=ranks)


epsilon = 1e-06

def reference(embeddings, cluster_ids, ranks):
    values = embeddings.astype(jnp.float32)
    unit = (values * lax.rsqrt(lax.optimization_barrier(jnp.sum(values * values, axis=1, keepdims=True)) + epsilon)).astype(jnp.bfloat16)
    cluster = cluster_ids[:, 0].astype(jnp.int32)
    row_order = jnp.argsort(cluster, stable=True).astype(jnp.int32)
    sorted_cluster = cluster[row_order]
    sorted_unit = unit[row_order]
    sorted_rank = ranks[row_order]
    offsets = jnp.searchsorted(sorted_cluster, jnp.arange(CLUSTERS, dtype=jnp.int32)).astype(jnp.int32)
    padded_unit = jnp.concatenate([sorted_unit, jnp.zeros((WINDOW, unit.shape[1]), jnp.bfloat16)], axis=0)
    padded_cluster = jnp.concatenate([sorted_cluster, jnp.full((WINDOW,), -1, jnp.int32)], axis=0)
    padded_rank = jnp.concatenate([sorted_rank, jnp.full((WINDOW,), -1, jnp.int32)], axis=0)

    def per_cluster(which):
        offset = offsets[which]
        members = lax.dynamic_slice_in_dim(padded_unit, offset, WINDOW, 0)
        member_cluster = lax.dynamic_slice_in_dim(padded_cluster, offset, WINDOW, 0)
        member_rank = lax.dynamic_slice_in_dim(padded_rank, offset, WINDOW, 0)
        scores = jnp.dot(members, members.T, preferred_element_type=jnp.float32)
        allowed = (member_cluster == which)[None, :] & (member_rank[None, :] < member_rank[:, None])
        return lax.optimization_barrier(jnp.max(jnp.where(allowed, scores, jnp.float32(-1.0)), axis=1))
    results = lax.map(per_cluster, jnp.arange(CLUSTERS, dtype=jnp.int32))
    position = jnp.arange(sorted_cluster.shape[0], dtype=jnp.int32) - offsets[sorted_cluster]
    sorted_result = results[sorted_cluster, position]
    return jnp.zeros((cluster.shape[0],), jnp.float32).at[row_order].set(sorted_result)
```

```python
import functools

import jax
import jax.numpy as jnp
from jax import lax
from jax.experimental import pallas as pl
from jax.experimental.pallas import tpu as pltpu
from jax.sharding import PartitionSpec as P

CLUSTERS = 256
CAP = 4
LANES = 128
TILE = 16

epsilon = 1e-06
EXACT = lax.Precision.HIGHEST
NN = (((1,), (0,)), ((), ()))
NT = (((1,), (1,)), ((), ()))
TN = (((0,), (0,)), ((), ()))
QUARTERS = (2, 1, 3, 0)


def dot(a, b, dims, precision=None):
    return lax.dot_general(a, b, dims, precision=precision, preferred_element_type=jnp.float32)


def iota(shape, axis):
    return lax.broadcasted_iota(jnp.int32, shape, axis)


def column(row):
    return jnp.transpose(jnp.broadcast_to(row, (LANES, row.shape[1])))[:, :1]


def kernel(n, splits, chunks, big, emb_hbm, cid_hbm, rank_hbm, out_ref, over_ref, *scratch):
    pieces = len(chunks)
    rows_out, rows_in = scratch[:pieces], scratch[pieces : 2 * pieces]
    (
        keys_out, keys_in, best_out, best_in,
        rows_out_sem, rows_in_sem, keys_out_sem, keys_in_sem, best_out_sem, best_in_sem, own_sem,
        emb_ref, cid_ref, rank_ref, load_sem,
    ) = scratch[2 * pieces :]
    me = lax.axis_index("loader") * splits + lax.axis_index("split")
    count, width = emb_hbm.shape
    quarter = n // 4
    mine, inner = me // quarter, me % quarter
    sign = 1 - 2 * (mine // 2)
    starts = [sum(chunks[:i]) for i in range(pieces)]

    def where_is(index):
        return {"loader": index // splits, "split": index % splits}

    def quarter_of(turn):
        return (mine + sign * QUARTERS[turn] + 4) % 4

    def each(act, turns=range(4)):
        for turn in turns:
            base = quarter_of(turn) * quarter
            first = 1 if QUARTERS[turn] == 0 else 0

            def step(i, carry):
                act(base + (inner + i) % quarter)
                return carry

            lax.fori_loop(first, quarter, step, 0)

    def remote(source, target, send, receive, peer):
        return pltpu.make_async_remote_copy(
            src_ref=source, dst_ref=target, send_sem=send, recv_sem=receive,
            device_id=where_is(peer), device_id_type=pl.DeviceIdType.MESH,
        )

    barrier = pltpu.get_barrier_semaphore()
    each(
        lambda peer: pl.semaphore_signal(
            barrier, inc=1, device_id=where_is(peer), device_id_type=pl.DeviceIdType.MESH
        )
    )

    loads = [
        pltpu.make_async_copy(source, target, load_sem.at[i])
        for i, (source, target) in enumerate(
            ((cid_hbm, cid_ref), (rank_hbm, rank_ref), (emb_hbm, emb_ref))
        )
    ]
    for load in loads:
        load.start()
    loads[0].wait()

    owner = cid_ref[...] % n
    before = (column(owner) == owner) & (iota((count, count), 0) < iota((count, count), 1))
    place = jnp.sum(before.astype(jnp.int32), axis=0, keepdims=True)
    owner_hot = iota((n, count), 0) == owner
    lane_hot = iota((LANES, count), 0) == place

    loads[1].wait()
    key = ((cid_ref[...] // n) * big + rank_ref[...] + 1).astype(jnp.float32)
    keys = dot(jnp.where(owner_hot, key, 0.0), lane_hot.astype(jnp.float32), NT, EXACT)
    lanes = iota((n, LANES), 1)
    missed = jnp.max(jnp.where(place >= sum(chunks), 1.0, 0.0), axis=1, keepdims=True)
    keys = jnp.where(lanes < sum(chunks), keys, jnp.where(lanes == LANES - 1, missed, 0.0))
    keys_out[...] = keys.reshape(n, 1, LANES)

    loads[2].wait()
    values = emb_ref[...].astype(jnp.float32)
    unit = (
        values * lax.rsqrt(jnp.sum(values * values, axis=1, keepdims=True) + epsilon)
    ).astype(jnp.bfloat16)

    def pack(piece, turn):
        size = chunks[piece]
        base = quarter_of(turn) * quarter
        local = place - starts[piece]
        slot = jnp.where((local >= 0) & (local < size), (owner - base) * size + local, -1)
        hot = (iota((quarter * size, count), 0) == slot).astype(jnp.bfloat16)
        packed = dot(hot, unit, NN).astype(jnp.bfloat16)
        rows_out[piece][pl.ds(base, quarter)] = packed.reshape(quarter, size, width)

    def send_keys(peer):
        return remote(
            keys_out.at[peer], keys_in.at[me], keys_out_sem, keys_in_sem, peer
        )

    others = pl.ds(0, n - 1)
    next_one = (me + 1) % n

    def take_keys():
        return remote(
            keys_out.at[others], keys_in.at[others], keys_out_sem, keys_in_sem, next_one
        )

    def send_rows(piece, peer):
        return remote(
            rows_out[piece].at[peer], rows_in[piece].at[me],
            rows_out_sem.at[piece], rows_in_sem.at[piece], peer,
        )

    def take_rows(piece):
        return remote(
            rows_out[piece].at[others], rows_in[piece].at[others],
            rows_out_sem.at[piece], rows_in_sem.at[piece], next_one,
        )

    def send_best(peer):
        return remote(
            best_out.at[peer], best_in.at[me], best_out_sem, best_in_sem, peer
        )

    def take_best():
        return remote(
            best_out.at[others], best_in.at[others], best_out_sem, best_in_sem, next_one
        )

    own = [
        pltpu.make_async_copy(rows_out[piece].at[me], rows_in[piece].at[me], own_sem.at[piece])
        for piece in range(pieces)
    ]
    own_keys = pltpu.make_async_copy(keys_out.at[me], keys_in.at[me], own_sem.at[pieces])
    own_best = pltpu.make_async_copy(best_out.at[me], best_in.at[me], own_sem.at[pieces + 1])

    for turn in range(4):
        pack(0, turn)
    pl.semaphore_wait(barrier, n - 1)
    for piece in range(pieces):
        for turn in range(4):
            if piece > 0:
                pack(piece, turn)
            each(lambda peer: send_rows(piece, peer).start(), (turn,))
        own[piece].start()
        if piece == 0:
            each(lambda peer: send_keys(peer).start())
            own_keys.start()

    take_keys().wait_recv()
    own_keys.wait()
    got = keys_in[...].reshape(n, LANES)
    over_ref[0, 0] = jnp.max(jnp.where(lanes == LANES - 1, got, 0.0))
    key_rows, key_columns, floors, spreads, sources = [], [], [], [], []
    for size, start in zip(chunks, starts):
        block = n * size
        source = (iota((n, block), 1) // size == iota((n, block), 0)).astype(jnp.float32)
        spread = iota((LANES, block), 0) == iota((LANES, block), 1) % size + start
        by_lane = dot(got, source, TN, EXACT)
        row = jnp.sum(jnp.where(spread, by_lane, 0.0), axis=0, keepdims=True)
        key_rows.append(row)
        key_columns.append(column(row))
        floors.append(jnp.floor(row * (1.0 / big)) * big)
        spreads.append(spread.astype(jnp.float32))
        sources.append(source)

    best = [jnp.full((1, n * size), -1.0, jnp.float32) for size in chunks]
    for piece, size in enumerate(chunks):
        take_rows(piece).wait_recv()
        own[piece].wait()
        here = rows_in[piece][...].reshape(n * size, width)
        for other in range(piece + 1):
            there = rows_in[other][...].reshape(n * chunks[other], width)
            pairs = [(here, piece, there, other)]
            if other != piece:
                pairs.append((there, other, here, piece))
            for members, m, queries, q in pairs:
                scores = dot(members, queries, NT)
                allowed = (key_columns[m] > floors[q]) & (key_columns[m] < key_rows[q])
                top = jnp.max(jnp.where(allowed, scores, -1.0), axis=0, keepdims=True)
                best[q] = jnp.maximum(best[q], top)
    answer = jnp.zeros((n, LANES), jnp.float32)
    for piece in range(pieces):
        answer = answer + dot(sources[piece] * best[piece], spreads[piece], NT, EXACT)
    best_out[...] = answer.reshape(n, 1, LANES)
    each(lambda peer: send_best(peer).start(), (2, 0, 1, 3))
    own_best.start()

    take_keys().wait_send()
    for piece in range(pieces):
        take_rows(piece).wait_send()
    take_best().wait_recv()
    own_best.wait()
    by_row = dot(best_in[...].reshape(n, LANES), owner_hot.astype(jnp.float32), TN, EXACT)
    out_ref[...] = jnp.sum(jnp.where(lane_hot, by_row, 0.0), axis=0, keepdims=True)
    take_best().wait_send()


def exchange(embeddings, cluster_ids, ranks, chunks, number):
    splits = lax.axis_size("split")
    n = lax.axis_size("loader") * splits
    count, width = embeddings.shape
    big = 1 << (n * count + 1).bit_length()
    dma = pltpu.SemaphoreType.DMA
    vmem = pl.BlockSpec(memory_space=pltpu.VMEM)
    rows = [pltpu.VMEM((n, size, width), jnp.bfloat16) for size in chunks]
    return pl.pallas_call(
        functools.partial(kernel, n, splits, chunks, big),
        out_shape=(
            jax.ShapeDtypeStruct((1, count), jnp.float32),
            jax.ShapeDtypeStruct((1, 1), jnp.float32),
        ),
        in_specs=[pl.BlockSpec(memory_space=pl.ANY)] * 3,
        out_specs=(vmem, pl.BlockSpec(memory_space=pltpu.SMEM)),
        scratch_shapes=[
            *rows,
            *rows,
            *[pltpu.VMEM((n, 1, LANES), jnp.float32)] * 4,
            dma((len(chunks),)),
            dma((len(chunks),)),
            *[dma] * 4,
            dma((len(chunks) + 2,)),
            pltpu.VMEM((count, width), embeddings.dtype),
            pltpu.VMEM((1, count), jnp.int32),
            pltpu.VMEM((1, count), jnp.int32),
            dma((3,)),
        ],
        compiler_params=pltpu.CompilerParams(collective_id=number, has_side_effects=True, vmem_limit_bytes=None if number == 0 else 67_043_328),
    )(embeddings, cluster_ids, ranks)


def two_sizes(embeddings, cluster_ids, ranks):
    n = lax.axis_size("loader") * lax.axis_size("split")
    count = embeddings.shape[0]
    cluster_ids, ranks = cluster_ids.reshape(1, count), ranks.reshape(1, count)
    most = CLUSTERS // n * CAP
    small, over = exchange(embeddings, cluster_ids, ranks, (TILE, most * 3 // 4 - TILE), 0)
    out = lax.cond(
        over[0, 0] > 0.0,
        lambda: exchange(embeddings, cluster_ids, ranks, (TILE, most - TILE), 1)[0],
        lambda: small,
    )
    return out.reshape(count)


def tile_scores(queries, remote):
    return jnp.einsum("kqd,kmd->kqm", queries, remote, preferred_element_type=jnp.float32)


def row_maxima(scores, query_rank, member_rank):
    allowed = (member_rank[:, None, :] >= 0) & (member_rank[:, None, :] < query_rank[:, :, None])
    return jnp.max(jnp.where(allowed, scores, jnp.float32(-1.0)), axis=2)


def small_tiles(embeddings, cluster_ids, ranks):
    loader_count = lax.axis_size("loader")
    split_count = lax.axis_size("split")
    rows_here = embeddings.shape[0]
    width = embeddings.shape[1]
    values = embeddings.astype(jnp.float32)
    unit = (values * lax.rsqrt(jnp.sum(values * values, axis=1, keepdims=True) + epsilon)).astype(
        jnp.bfloat16
    )
    cluster = cluster_ids[:, 0]
    row_index = jnp.arange(rows_here, dtype=jnp.int32)
    same_cluster = cluster[:, None] == cluster[None, :]
    earlier = row_index[None, :] < row_index[:, None]
    position = jnp.sum((same_cluster & earlier).astype(jnp.int32), axis=1)
    slot_count = CLUSTERS * CAP
    device_count = loader_count * split_count
    owner_flat = cluster % device_count
    cluster_slot = cluster // device_count
    owned = CLUSTERS // device_count
    target = (
        (cluster_slot * loader_count + owner_flat // split_count) * split_count
        + owner_flat % split_count
    ) * CAP + position
    send_rows = (
        jnp.zeros((slot_count, width), jnp.bfloat16)
        .at[target]
        .set(unit)
        .reshape(owned, loader_count, split_count, CAP, width)
    )
    send_rank = (
        jnp.full((slot_count,), -1, jnp.int32)
        .at[target]
        .set(ranks)
        .reshape(owned, loader_count, split_count, CAP)
    )

    def swap(block):
        return lax.all_to_all(
            lax.all_to_all(block, "loader", split_axis=1, concat_axis=1, tiled=True),
            "split",
            split_axis=2,
            concat_axis=2,
            tiled=True,
        )

    members = swap(send_rows).reshape(owned, -1, width)
    member_rank = swap(send_rank).reshape(owned, -1)
    best = row_maxima(tile_scores(members, members), member_rank, member_rank)
    returned = swap(best.reshape(owned, loader_count, split_count, CAP))
    return returned.reshape(-1)[target]


def shards(embeddings, cluster_ids, ranks):
    n = lax.axis_size("loader") * lax.axis_size("split")
    fits = n % 4 == 0 and CLUSTERS // n * CAP == 2 * TILE
    return (two_sizes if fits else small_tiles)(embeddings, cluster_ids, ranks)


def solution(mesh):
    return jax.shard_map(
        shards,
        mesh=mesh,
        in_specs=(
            P(("loader", "split"), None),
            P(("loader", "split"), None),
            P(("loader", "split")),
        ),
        out_specs=P(("loader", "split")),
        check_vma=False,
    )
```

```python
import functools

import jax
import jax.numpy as jnp
from jax import lax
from jax.experimental import pallas as pl
from jax.experimental.pallas import tpu as pltpu
from jax.sharding import PartitionSpec as P

CLUSTERS = 256
CAP = 4
LANES = 128
TILE = 16

epsilon = 1e-06
EXACT = lax.Precision.HIGHEST
NN = (((1,), (0,)), ((), ()))
NT = (((1,), (1,)), ((), ()))
TN = (((0,), (0,)), ((), ()))
QUARTERS = (2, 1, 3, 0)


def dot(a, b, dims, precision=None):
    return lax.dot_general(a, b, dims, precision=precision, preferred_element_type=jnp.float32)


def iota(shape, axis):
    return lax.broadcasted_iota(jnp.int32, shape, axis)


def column(row):
    return jnp.transpose(jnp.broadcast_to(row, (LANES, row.shape[1])))[:, :1]


def kernel(n, splits, chunks, big, emb_hbm, cid_hbm, rank_hbm, out_ref, over_ref, *scratch):
    pieces = len(chunks)
    rows_out, rows_in = scratch[:pieces], scratch[pieces : 2 * pieces]
    (
        keys_out, keys_in, best_out, best_in,
        rows_out_sem, rows_in_sem, keys_out_sem, keys_in_sem, best_out_sem, best_in_sem, own_sem,
        emb_ref, cid_ref, rank_ref, load_sem,
    ) = scratch[2 * pieces :]
    me = lax.axis_index("loader") * splits + lax.axis_index("split")
    count, width = emb_hbm.shape
    quarter = n // 4
    mine, inner = me // quarter, me % quarter
    sign = 1 - 2 * (mine // 2)
    starts = [sum(chunks[:i]) for i in range(pieces)]

    def where_is(index):
        return {"loader": index // splits, "split": index % splits}

    def quarter_of(turn):
        return (mine + sign * QUARTERS[turn] + 4) % 4

    def each(act, turns=range(4)):
        for turn in turns:
            base = quarter_of(turn) * quarter
            first = 1 if QUARTERS[turn] == 0 else 0

            def step(i, carry):
                act(base + (inner + i) % quarter)
                return carry

            lax.fori_loop(first, quarter, step, 0)

    def remote(source, target, send, receive, peer):
        return pltpu.make_async_remote_copy(
            src_ref=source, dst_ref=target, send_sem=send, recv_sem=receive,
            device_id=where_is(peer), device_id_type=pl.DeviceIdType.MESH,
        )

    barrier = pltpu.get_barrier_semaphore()
    each(
        lambda peer: pl.semaphore_signal(
            barrier, inc=1, device_id=where_is(peer), device_id_type=pl.DeviceIdType.MESH
        )
    )

    loads = [
        pltpu.make_async_copy(source, target, load_sem.at[i])
        for i, (source, target) in enumerate(
            ((cid_hbm, cid_ref), (rank_hbm, rank_ref), (emb_hbm, emb_ref))
        )
    ]
    for load in loads:
        load.start()
    loads[0].wait()

    owner = cid_ref[...] % n
    before = (column(owner) == owner) & (iota((count, count), 0) < iota((count, count), 1))
    place = jnp.sum(before.astype(jnp.int32), axis=0, keepdims=True)
    owner_hot = iota((n, count), 0) == owner
    lane_hot = iota((LANES, count), 0) == place

    loads[1].wait()
    key = ((cid_ref[...] // n) * big + rank_ref[...] + 1).astype(jnp.float32)
    keys = dot(jnp.where(owner_hot, key, 0.0), lane_hot.astype(jnp.float32), NT, EXACT)
    lanes = iota((n, LANES), 1)
    missed = jnp.max(jnp.where(place >= sum(chunks), 1.0, 0.0), axis=1, keepdims=True)
    keys = jnp.where(lanes < sum(chunks), keys, jnp.where(lanes == LANES - 1, missed, 0.0))
    keys_out[...] = keys.reshape(n, 1, LANES)

    loads[2].wait()
    values = emb_ref[...].astype(jnp.float32)
    unit = (
        values * lax.rsqrt(jnp.sum(values * values, axis=1, keepdims=True) + epsilon)
    ).astype(jnp.bfloat16)

    def pack(piece, turn):
        size = chunks[piece]
        base = quarter_of(turn) * quarter
        local = place - starts[piece]
        slot = jnp.where((local >= 0) & (local < size), (owner - base) * size + local, -1)
        hot = (iota((quarter * size, count), 0) == slot).astype(jnp.bfloat16)
        packed = dot(hot, unit, NN).astype(jnp.bfloat16)
        rows_out[piece][pl.ds(base, quarter)] = packed.reshape(quarter, size, width)

    def send_keys(peer):
        return remote(
            keys_out.at[peer], keys_in.at[me], keys_out_sem, keys_in_sem, peer
        )

    others = pl.ds(0, n - 1)
    next_one = (me + 1) % n

    def take_keys():
        return remote(
            keys_out.at[others], keys_in.at[others], keys_out_sem, keys_in_sem, next_one
        )

    def send_rows(piece, peer):
        return remote(
            rows_out[piece].at[peer], rows_in[piece].at[me],
            rows_out_sem.at[piece], rows_in_sem.at[piece], peer,
        )

    def take_rows(piece):
        return remote(
            rows_out[piece].at[others], rows_in[piece].at[others],
            rows_out_sem.at[piece], rows_in_sem.at[piece], next_one,
        )

    def send_best(peer):
        return remote(
            best_out.at[peer], best_in.at[me], best_out_sem, best_in_sem, peer
        )

    def take_best():
        return remote(
            best_out.at[others], best_in.at[others], best_out_sem, best_in_sem, next_one
        )

    own = [
        pltpu.make_async_copy(rows_out[piece].at[me], rows_in[piece].at[me], own_sem.at[piece])
        for piece in range(pieces)
    ]
    own_keys = pltpu.make_async_copy(keys_out.at[me], keys_in.at[me], own_sem.at[pieces])
    own_best = pltpu.make_async_copy(best_out.at[me], best_in.at[me], own_sem.at[pieces + 1])

    for turn in range(4):
        pack(0, turn)
    pl.semaphore_wait(barrier, n - 1)
    for piece in range(pieces):
        for turn in range(4):
            if piece > 0:
                pack(piece, turn)
            each(lambda peer: send_rows(piece, peer).start(), (turn,))
        own[piece].start()
        if piece == 0:
            each(lambda peer: send_keys(peer).start())
            own_keys.start()

    take_keys().wait_recv()
    own_keys.wait()
    got = keys_in[...].reshape(n, LANES)
    over_ref[0, 0] = jnp.max(jnp.where(lanes == LANES - 1, got, 0.0))
    key_rows, key_columns, floors, spreads, sources = [], [], [], [], []
    for size, start in zip(chunks, starts):
        block = n * size
        source = (iota((n, block), 1) // size == iota((n, block), 0)).astype(jnp.float32)
        spread = iota((LANES, block), 0) == iota((LANES, block), 1) % size + start
        by_lane = dot(got, source, TN, EXACT)
        row = jnp.sum(jnp.where(spread, by_lane, 0.0), axis=0, keepdims=True)
        key_rows.append(row)
        key_columns.append(column(row))
        floors.append(jnp.floor(row * (1.0 / big)) * big)
        spreads.append(spread.astype(jnp.float32))
        sources.append(source)

    best = [jnp.full((1, n * size), -1.0, jnp.float32) for size in chunks]
    for piece, size in enumerate(chunks):
        take_rows(piece).wait_recv()
        own[piece].wait()
        here = rows_in[piece][...].reshape(n * size, width)
        for other in range(piece + 1):
            there = rows_in[other][...].reshape(n * chunks[other], width)
            pairs = [(here, piece, there, other)]
            if other != piece:
                pairs.append((there, other, here, piece))
            for members, m, queries, q in pairs:
                scores = dot(members, queries, NT)
                allowed = (key_columns[m] > floors[q]) & (key_columns[m] < key_rows[q])
                top = jnp.max(jnp.where(allowed, scores, -1.0), axis=0, keepdims=True)
                best[q] = jnp.maximum(best[q], top)
    answer = jnp.zeros((n, LANES), jnp.float32)
    for piece in range(pieces):
        answer = answer + dot(sources[piece] * best[piece], spreads[piece], NT, EXACT)
    best_out[...] = answer.reshape(n, 1, LANES)
    each(lambda peer: send_best(peer).start(), (2, 0, 1, 3))
    own_best.start()

    take_keys().wait_send()
    for piece in range(pieces):
        take_rows(piece).wait_send()
    take_best().wait_recv()
    own_best.wait()
    by_row = dot(best_in[...].reshape(n, LANES), owner_hot.astype(jnp.float32), TN, EXACT)
    out_ref[...] = jnp.sum(jnp.where(lane_hot, by_row, 0.0), axis=0, keepdims=True)
    take_best().wait_send()


def exchange(embeddings, cluster_ids, ranks, chunks, number):
    splits = lax.axis_size("split")
    n = lax.axis_size("loader") * splits
    count, width = embeddings.shape
    big = 1 << (n * count + 1).bit_length()
    dma = pltpu.SemaphoreType.DMA
    vmem = pl.BlockSpec(memory_space=pltpu.VMEM)
    rows = [pltpu.VMEM((n, size, width), jnp.bfloat16) for size in chunks]
    return pl.pallas_call(
        functools.partial(kernel, n, splits, chunks, big),
        out_shape=(
            jax.ShapeDtypeStruct((1, count), jnp.float32),
            jax.ShapeDtypeStruct((1, 1), jnp.float32),
        ),
        in_specs=[pl.BlockSpec(memory_space=pl.ANY)] * 3,
        out_specs=(vmem, pl.BlockSpec(memory_space=pltpu.SMEM)),
        scratch_shapes=[
            *rows,
            *rows,
            *[pltpu.VMEM((n, 1, LANES), jnp.float32)] * 4,
            dma((len(chunks),)),
            dma((len(chunks),)),
            *[dma] * 4,
            dma((len(chunks) + 2,)),
            pltpu.VMEM((count, width), embeddings.dtype),
            pltpu.VMEM((1, count), jnp.int32),
            pltpu.VMEM((1, count), jnp.int32),
            dma((3,)),
        ],
        compiler_params=pltpu.CompilerParams(collective_id=number, has_side_effects=True, vmem_limit_bytes=None if number == 0 else 67_043_328),
    )(embeddings, cluster_ids, ranks)


PLANES = 4
POOL = 20
STRIP = 4
EXTRA = 8


def pooled_kernel(
    n, splits, big, emb_hbm, cid_hbm, rank_hbm, out_ref, over_ref,
    emb_ref, cid_ref, rank_ref, rows_out, rows_in, pool_out, pool_in, extra_out, extra_in,
    meta_out, meta_in, keys_out, keys_in, best_out, best_in,
    load_sem, rows_out_sem, rows_in_sem, pool_sem, meta_sem, extra_sem, keys_sem, best_sem, ready,
):
    me = lax.axis_index("loader") * splits + lax.axis_index("split")
    count, width = emb_hbm.shape
    wide = n // PLANES
    z, j = me // wide, me % wide
    upper = z // 2
    farthest = 3 - 3 * upper
    order = (farthest, farthest - 1 + 2 * upper, 1 - z + 4 * upper, z)
    rows_of = wide // splits
    chip = j // 2

    def position(inner):
        return inner, inner // splits, inner % splits

    def near(turn, core):
        other = chip + turn
        return position(2 * jnp.where(other >= wide // 2, other - wide // 2, other) + core)

    partner = position(j + 1 - 2 * (j % 2))
    column_pair = (position(j), partner)
    around = [near(turn, core) for turn in range(1, wide // 2) for core in range(2)]

    def at(plane, spot):
        return plane * wide + spot[0], {"loader": plane * rows_of + spot[1], "split": spot[2]}

    def everyone(act):
        for peer in range(n):
            where = {"loader": peer // splits, "split": peer % splits}
            pl.when(me != peer)(functools.partial(act, peer, where))

    def remote(source, target, send, receive, peer):
        return pltpu.make_async_remote_copy(
            src_ref=source, dst_ref=target, send_sem=send, recv_sem=receive,
            device_id=peer, device_id_type=pl.DeviceIdType.MESH,
        )

    def signal(semaphore, peer):
        pl.semaphore_signal(semaphore, inc=1, device_id=peer, device_id_type=pl.DeviceIdType.MESH)

    barrier = pltpu.get_barrier_semaphore()
    for turn in range(3):
        for spot in column_pair:
            signal(barrier, at(order[turn], spot)[1])
    for spot in (partner, *around):
        signal(barrier, at(z, spot)[1])

    bands = 4
    band = count // bands
    pairs = [(cid_hbm, cid_ref), (rank_hbm, rank_ref)]
    for i in range(bands):
        rows = pl.ds(i * band, band)
        pairs.append((emb_hbm.at[rows], emb_ref.at[rows]))
    loads = [
        pltpu.make_async_copy(source, target, load_sem.at[i])
        for i, (source, target) in enumerate(pairs)
    ]
    for load in (loads[0], *loads[2:], loads[1]):
        load.start()
    earlier = (iota((count, count), 0) < iota((count, count), 1)).astype(jnp.bfloat16)
    loads[0].wait()

    owner = cid_ref[...] % n
    plane = owner // wide
    owner_hot = iota((n, count), 0) == owner
    so_far = dot(owner_hot.astype(jnp.bfloat16), earlier, NN)
    place = jnp.sum(jnp.where(owner_hot, so_far, 0.0), axis=0, keepdims=True).astype(jnp.int32)
    spill = jnp.maximum(so_far - TILE, 0.0)
    pooled = jnp.zeros((1, count), jnp.float32)
    for p in range(PLANES):
        here = jnp.sum(spill[p * wide : (p + 1) * wide], axis=0, keepdims=True)
        pooled = jnp.where(plane == p, here, pooled)
    pooled = pooled.astype(jnp.int32)
    spilled = place >= TILE
    fits = (place < TILE + EXTRA) & (pooled < POOL)
    turned = (z + 2 * PLANES - 1 - plane) % PLANES
    pool_row = jnp.where(spilled & fits, turned * POOL + pooled, -1)
    pool_hot = (iota((LANES, count), 0) == pool_row).astype(jnp.bfloat16)
    units = []
    for i in range(bands):
        loads[2 + i].wait()
        values = emb_ref[i * band : (i + 1) * band].astype(jnp.float32)
        scale = lax.rsqrt(jnp.sum(values * values, axis=1, keepdims=True) + epsilon)
        units.append((values * scale).astype(jnp.bfloat16))
    unit = jnp.concatenate(units, axis=0)
    strips = POOL // STRIP
    pool = dot(pool_hot[: PLANES * POOL], unit, NN).astype(jnp.bfloat16)
    pool_out[...] = pool.reshape(PLANES * strips, STRIP, width)
    own_pool = pl.ds((PLANES - 1) * strips, strips)
    pool_in[own_pool] = pool_out[own_pool]
    slot = jnp.where(spilled, -1, owner * TILE + place)

    def pack(plane):
        size = wide * TILE
        hot = (iota((size, count), 0) + plane * size == slot).astype(jnp.bfloat16)
        packed = dot(hot, unit, NN).astype(jnp.bfloat16)
        rows_out[pl.ds(plane * wide, wide)] = packed.reshape(wide, TILE, width)

    def send_rows(plane, spots):
        for spot in spots:
            peer, where = at(plane, spot)
            remote(
                rows_out.at[peer], rows_in.at[me], rows_out_sem, rows_in_sem.at[z], where
            ).start()

    others = pl.ds(0, n - 1)
    next_one = at(z, partner)[1]
    pools = pl.ds(0, (PLANES - 1) * strips)
    fellows = pl.ds(0, wide - 1)
    take_pools = remote(
        pool_out.at[pools], pool_in.at[pools], pool_sem.at[0], pool_sem.at[1], next_one
    )
    take_meta = remote(
        meta_in.at[pl.ds(0, PLANES - 1)], meta_in.at[pl.ds(0, PLANES - 1)],
        meta_sem.at[0], meta_sem.at[1], next_one,
    )
    take_extra = remote(
        extra_out.at[fellows], extra_in.at[fellows], extra_sem.at[0], extra_sem.at[1], next_one
    )
    take_keys = remote(
        keys_out.at[others], keys_in.at[others], keys_sem.at[0], keys_sem.at[1], next_one
    )
    take_best = remote(
        best_in.at[others], best_in.at[others], best_sem.at[0], best_sem.at[1], next_one
    )
    sent_rows = remote(
        rows_out.at[others], rows_in.at[others], rows_out_sem, rows_in_sem.at[0], next_one
    )

    def take_rows(source, many):
        block = pl.ds(0, many)
        remote(
            rows_out.at[block], rows_in.at[block], rows_out_sem, rows_in_sem.at[source], next_one
        ).wait_recv()

    def send_pool(plane):
        step = (z + 2 * PLANES - 1 - plane) % PLANES
        block = pl.ds(step * strips, strips)
        where = at(plane, column_pair[0])[1]
        remote(
            pool_out.at[block], pool_in.at[block], pool_sem.at[0], pool_sem.at[1], where
        ).start()

    def send_meta(plane):
        step = (z + 2 * PLANES - 1 - plane) % PLANES
        where = at(plane, column_pair[0])[1]
        remote(meta_out, meta_in.at[step], meta_sem.at[0], meta_sem.at[1], where).start()

    pl.semaphore_wait(barrier, 2 * (PLANES - 1) + wide - 1)
    for turn in range(3):
        send_pool(order[turn])
    for spot in around:
        signal(ready, at(z, spot)[1])
    code = ((owner % wide) * EXTRA + place - TILE + 1).astype(jnp.float32)
    code = jnp.broadcast_to(jnp.where(spilled, code, 0.0), (8, count)).astype(jnp.bfloat16)
    meta_out[...] = dot(code, pool_hot, NT)[:1]
    meta_in[PLANES - 1] = meta_out[...]
    for turn in range(3):
        send_meta(order[turn])
    for turn in range(3):
        pack(order[turn])
        send_rows(order[turn], column_pair)
    pack(z)
    rows_in[me] = rows_out[me]
    send_rows(z, [partner, *around])
    loads[1].wait()
    lanes = iota((n, LANES), 1)
    lane_hot = iota((LANES, count), 0) == place
    key = ((cid_ref[...] // n) * big + rank_ref[...] + 1).astype(jnp.float32)
    keys = dot(jnp.where(owner_hot, key, 0.0), lane_hot.astype(jnp.float32), NT, EXACT)
    missed = jnp.max(jnp.where(spilled & ~fits, 1.0, 0.0), axis=1, keepdims=True)
    keys = jnp.where(lanes < TILE + EXTRA, keys, jnp.where(lanes == LANES - 1, missed, 0.0))
    keys_out[...] = keys.reshape(n, 1, LANES)
    pl.semaphore_wait(ready, wide - 2)

    def send_keys(peer, where):
        remote(
            keys_out.at[peer], keys_in.at[me], keys_sem.at[0], keys_sem.at[1], where
        ).start()

    everyone(send_keys)
    keys_in[me] = keys_out[me]

    take_meta.wait_recv()
    segment = iota((1, LANES), 1) // POOL
    codes = jnp.full((1, LANES), -1.0, jnp.float32)
    for step in range(PLANES):
        got = meta_in[step]
        codes = jnp.where((segment == step) & (got > 0.0), got + step * 128.0, codes)
    codes = codes[:, : PLANES * POOL]
    block = wide * PLANES * EXTRA
    shape = (block, PLANES * POOL)
    line = iota(shape, 0)
    wanted = (line // EXTRA % PLANES) * 128 + line // (PLANES * EXTRA) * EXTRA + line % EXTRA + 1
    expand = (wanted.astype(jnp.float32) == codes).astype(jnp.bfloat16)
    take_pools.wait_recv()
    send_rows(order[0], around)
    expanded = dot(expand, pool_in[...].reshape(PLANES * POOL, width), NN).astype(jnp.bfloat16)
    extra_out[...] = expanded.reshape(wide, PLANES * EXTRA, width)
    extra_in[j] = extra_out[j]

    for spot in (partner, *around):
        remote(
            extra_out.at[spot[0]], extra_in.at[j], extra_sem.at[0], extra_sem.at[1],
            at(z, spot)[1],
        ).start()
    send_rows(order[1], around)
    send_rows(order[2], around)

    take_keys.wait_recv()
    over_ref[0, 0] = jnp.max(jnp.where(lanes == LANES - 1, keys_in[...].reshape(n, LANES), 0.0))
    row = iota((wide, LANES), 0)

    def keys_of(source):
        return keys_in[pl.ds(source * wide, wide)].reshape(wide, LANES)

    def plane_keys(source):
        spread = pltpu.roll(keys_of(source), 0, 1, stride=TILE, stride_axis=0)
        mine = iota((wide, LANES), 1) // TILE == row
        return jnp.sum(jnp.where(mine, spread, 0.0), axis=0, keepdims=True)

    run = PLANES * EXTRA
    per_tile = LANES // run
    lane = iota((wide, LANES), 1)
    run_keys = jnp.zeros((wide, LANES), jnp.float32)
    for step in range(PLANES):
        got = keys_of((z + 1 + step) % PLANES)
        moved = pltpu.roll(got, (step * EXTRA - TILE) % LANES, 1)
        run_keys = jnp.where(lane // EXTRA == step, moved, run_keys)
    repeated = run_keys
    for turn in range(1, per_tile):
        repeated = repeated + pltpu.roll(run_keys, turn * run, 1)
    repeated = jnp.where(lane // run == row % per_tile, repeated, 0.0)
    halves = [
        jnp.sum(repeated[first : first + per_tile], axis=0, keepdims=True)
        for first in range(0, wide, per_tile)
    ]

    def keyed(line):
        return line, column(line), jnp.floor(line * (1.0 / big)) * big

    sources = (order[3], None, order[2], order[0], order[1])
    keyring, best = [], []
    for source in sources:
        if source is None:
            line = jnp.concatenate(halves, axis=1)
        else:
            line = plane_keys(source)
        keyring.append(keyed(line))
        best.append(jnp.full(line.shape, -1.0, jnp.float32))

    def fetch(index):
        if sources[index] is None:
            return extra_in[...].reshape(block, width)
        return rows_in[pl.ds(sources[index] * wide, wide)].reshape(wide * TILE, width)

    def score(members, m, queries, q):
        scores = dot(members, queries, NT)
        key_row, _, floor = keyring[q]
        key_column = keyring[m][1]
        allowed = (key_column > floor) & (key_column < key_row)
        top = jnp.max(jnp.where(allowed, scores, -1.0), axis=0, keepdims=True)
        best[q] = jnp.maximum(best[q], top)

    def arrive(index):
        if sources[index] is None:
            take_extra.wait_recv()
        else:
            take_rows(sources[index], wide - 1 if index == 0 else wide)

    def answer(index):
        plane = sources[index]
        for half in range(tiles):
            best_out[plane * tiles + half, 0:1] = best[index]
            best_out[plane * tiles + half, 1:2] = best[1][:, half * LANES : (half + 1) * LANES]

        def send_best(inner):
            peer, where = at(plane, (inner, inner // splits, inner % splits))
            remote(
                best_out.at[plane * tiles + inner // per_tile], best_in.at[me],
                best_sem.at[0], best_sem.at[1], where,
            ).start()

        for inner in range(wide):
            if index == 0:
                pl.when(j != inner)(functools.partial(send_best, inner))
            else:
                send_best(inner)

    tiles = wide // per_tile
    last = len(sources) - 1
    for index in range(last):
        arrive(index)
        new = fetch(index)
        for other in range(index):
            old = fetch(other)
            if index < 3 or other > 0:
                score(new, index, old, other)
            score(old, other, new, index)
        score(new, index, new, index)
    arrive(last)
    new = fetch(last)
    for other in (1, 3, 2, 0):
        if other == 0:
            score(fetch(3), 3, fetch(0), 0)
        score(new, last, fetch(other), other)
        if other != 1:
            answer(other)
    for other in range(last):
        score(fetch(other), other, new, last)
    score(new, last, new, last)
    answer(last)
    best_in[me] = best_out[z * tiles + j // per_tile]

    take_pools.wait_send()
    for step in range(PLANES - 1):
        remote(meta_out, meta_in.at[step], meta_sem.at[0], meta_sem.at[1], next_one).wait_send()
    take_keys.wait_send()
    take_extra.wait_send()
    sent_rows.wait_send()
    take_best.wait_recv()
    answers = pltpu.roll(best_in[:, 0, :], (LANES - j * TILE) % LANES, 1)
    spare = best_in[:, 1, :]
    shifted = []
    for p in range(PLANES):
        step = (z + 2 * PLANES - 1 - p) % PLANES
        begin = j % per_tile * PLANES * EXTRA + step * EXTRA
        shifted.append(
            pltpu.roll(spare[p * wide : (p + 1) * wide], (LANES + TILE - begin) % LANES, 1)
        )
    table = jnp.where(lanes < TILE, answers, jnp.concatenate(shifted, axis=0))
    kept = 2 * TILE
    by_row = dot(table[:, :kept], owner_hot.astype(jnp.float32), TN, EXACT)
    out_ref[...] = jnp.sum(jnp.where(lane_hot[:kept], by_row, 0.0), axis=0, keepdims=True)
    take_best.wait_send()


def pooled_exchange(embeddings, cluster_ids, ranks):
    splits = lax.axis_size("split")
    n = lax.axis_size("loader") * splits
    count, width = embeddings.shape
    big = 1 << (n * count + 1).bit_length()
    wide = n // PLANES
    dma = pltpu.SemaphoreType.DMA

    def held(*shape):
        return pltpu.VMEM(shape, jnp.bfloat16)

    def told(*shape):
        return pltpu.VMEM(shape, jnp.float32)

    return pl.pallas_call(
        functools.partial(pooled_kernel, n, splits, big),
        out_shape=(
            jax.ShapeDtypeStruct((1, count), jnp.float32),
            jax.ShapeDtypeStruct((1, 1), jnp.float32),
        ),
        in_specs=[pl.BlockSpec(memory_space=pl.ANY)] * 3,
        out_specs=(
            pl.BlockSpec(memory_space=pltpu.VMEM), pl.BlockSpec(memory_space=pltpu.SMEM)
        ),
        scratch_shapes=[
            pltpu.VMEM((count, width), embeddings.dtype),
            pltpu.VMEM((1, count), jnp.int32),
            pltpu.VMEM((1, count), jnp.int32),
            *[held(n, TILE, width)] * 2,
            *[held(PLANES * POOL // STRIP, STRIP, width)] * 2,
            *[held(wide, PLANES * EXTRA, width)] * 2,
            told(1, LANES),
            told(PLANES, 1, LANES),
            *[told(n, 1, LANES)] * 2,
            told(PLANES * (wide * PLANES * EXTRA // LANES), 2, LANES),
            told(n, 2, LANES),
            dma((6,)),
            dma,
            dma((PLANES,)),
            *[dma((2,))] * 5,
            pltpu.SemaphoreType.REGULAR,
        ],
        compiler_params=pltpu.CompilerParams(collective_id=0, has_side_effects=True),
    )(embeddings, cluster_ids, ranks)


def two_sizes(embeddings, cluster_ids, ranks):
    n = lax.axis_size("loader") * lax.axis_size("split")
    count = embeddings.shape[0]
    cluster_ids, ranks = cluster_ids.reshape(1, count), ranks.reshape(1, count)
    most = CLUSTERS // n * CAP
    small, over = pooled_exchange(embeddings, cluster_ids, ranks)
    out = lax.cond(
        over[0, 0] > 0.0,
        lambda: exchange(embeddings, cluster_ids, ranks, (TILE, most - TILE), 1)[0],
        lambda: small,
    )
    return out.reshape(count)


def tile_scores(queries, remote):
    return jnp.einsum("kqd,kmd->kqm", queries, remote, preferred_element_type=jnp.float32)


def row_maxima(scores, query_rank, member_rank):
    allowed = (member_rank[:, None, :] >= 0) & (member_rank[:, None, :] < query_rank[:, :, None])
    return jnp.max(jnp.where(allowed, scores, jnp.float32(-1.0)), axis=2)


def small_tiles(embeddings, cluster_ids, ranks):
    loader_count = lax.axis_size("loader")
    split_count = lax.axis_size("split")
    rows_here = embeddings.shape[0]
    width = embeddings.shape[1]
    values = embeddings.astype(jnp.float32)
    unit = (values * lax.rsqrt(jnp.sum(values * values, axis=1, keepdims=True) + epsilon)).astype(
        jnp.bfloat16
    )
    cluster = cluster_ids[:, 0]
    row_index = jnp.arange(rows_here, dtype=jnp.int32)
    same_cluster = cluster[:, None] == cluster[None, :]
    earlier = row_index[None, :] < row_index[:, None]
    position = jnp.sum((same_cluster & earlier).astype(jnp.int32), axis=1)
    slot_count = CLUSTERS * CAP
    device_count = loader_count * split_count
    owner_flat = cluster % device_count
    cluster_slot = cluster // device_count
    owned = CLUSTERS // device_count
    target = (
        (cluster_slot * loader_count + owner_flat // split_count) * split_count
        + owner_flat % split_count
    ) * CAP + position
    send_rows = (
        jnp.zeros((slot_count, width), jnp.bfloat16)
        .at[target]
        .set(unit)
        .reshape(owned, loader_count, split_count, CAP, width)
    )
    send_rank = (
        jnp.full((slot_count,), -1, jnp.int32)
        .at[target]
        .set(ranks)
        .reshape(owned, loader_count, split_count, CAP)
    )

    def swap(block):
        return lax.all_to_all(
            lax.all_to_all(block, "loader", split_axis=1, concat_axis=1, tiled=True),
            "split",
            split_axis=2,
            concat_axis=2,
            tiled=True,
        )

    members = swap(send_rows).reshape(owned, -1, width)
    member_rank = swap(send_rank).reshape(owned, -1)
    best = row_maxima(tile_scores(members, members), member_rank, member_rank)
    returned = swap(best.reshape(owned, loader_count, split_count, CAP))
    return returned.reshape(-1)[target]


def shards(embeddings, cluster_ids, ranks):
    n = lax.axis_size("loader") * lax.axis_size("split")
    fits = n % 4 == 0 and CLUSTERS // n * CAP == 2 * TILE
    return (two_sizes if fits else small_tiles)(embeddings, cluster_ids, ranks)


def solution(mesh):
    return jax.shard_map(
        shards,
        mesh=mesh,
        in_specs=(
            P(("loader", "split"), None),
            P(("loader", "split"), None),
            P(("loader", "split")),
        ),
        out_specs=P(("loader", "split")),
        check_vma=False,
    )
```

```python
import functools

import jax
import jax.numpy as jnp
from jax import lax
from jax.experimental import pallas as pl
from jax.experimental.pallas import tpu as pltpu
from jax.sharding import PartitionSpec as P

CLUSTERS = 256
CAP = 4
LANES = 128
TILE = 16

epsilon = 1e-06
EXACT = lax.Precision.HIGHEST
NN = (((1,), (0,)), ((), ()))
NT = (((1,), (1,)), ((), ()))
TN = (((0,), (0,)), ((), ()))
QUARTERS = (2, 1, 3, 0)


def dot(a, b, dims, precision=None):
    return lax.dot_general(a, b, dims, precision=precision, preferred_element_type=jnp.float32)


def iota(shape, axis):
    return lax.broadcasted_iota(jnp.int32, shape, axis)


def column(row):
    return jnp.transpose(jnp.broadcast_to(row, (LANES, row.shape[1])))[:, :1]


def kernel(n, splits, chunks, big, emb_hbm, cid_hbm, rank_hbm, out_ref, over_ref, *scratch):
    pieces = len(chunks)
    rows_out, rows_in = scratch[:pieces], scratch[pieces : 2 * pieces]
    (
        keys_out, keys_in, best_out, best_in,
        rows_out_sem, rows_in_sem, keys_out_sem, keys_in_sem, best_out_sem, best_in_sem, own_sem,
        emb_ref, cid_ref, rank_ref, load_sem,
    ) = scratch[2 * pieces :]
    me = lax.axis_index("loader") * splits + lax.axis_index("split")
    count, width = emb_hbm.shape
    quarter = n // 4
    mine, inner = me // quarter, me % quarter
    sign = 1 - 2 * (mine // 2)
    starts = [sum(chunks[:i]) for i in range(pieces)]

    def where_is(index):
        return {"loader": index // splits, "split": index % splits}

    def quarter_of(turn):
        return (mine + sign * QUARTERS[turn] + 4) % 4

    def each(act, turns=range(4)):
        for turn in turns:
            base = quarter_of(turn) * quarter
            first = 1 if QUARTERS[turn] == 0 else 0

            def step(i, carry):
                act(base + (inner + i) % quarter)
                return carry

            lax.fori_loop(first, quarter, step, 0)

    def remote(source, target, send, receive, peer):
        return pltpu.make_async_remote_copy(
            src_ref=source, dst_ref=target, send_sem=send, recv_sem=receive,
            device_id=where_is(peer), device_id_type=pl.DeviceIdType.MESH,
        )

    barrier = pltpu.get_barrier_semaphore()
    each(
        lambda peer: pl.semaphore_signal(
            barrier, inc=1, device_id=where_is(peer), device_id_type=pl.DeviceIdType.MESH
        )
    )

    loads = [
        pltpu.make_async_copy(source, target, load_sem.at[i])
        for i, (source, target) in enumerate(
            ((cid_hbm, cid_ref), (rank_hbm, rank_ref), (emb_hbm, emb_ref))
        )
    ]
    for load in loads:
        load.start()
    loads[0].wait()

    owner = cid_ref[...] % n
    before = (column(owner) == owner) & (iota((count, count), 0) < iota((count, count), 1))
    place = jnp.sum(before.astype(jnp.int32), axis=0, keepdims=True)
    owner_hot = iota((n, count), 0) == owner
    lane_hot = iota((LANES, count), 0) == place

    loads[1].wait()
    key = ((cid_ref[...] // n) * big + rank_ref[...] + 1).astype(jnp.float32)
    keys = dot(jnp.where(owner_hot, key, 0.0), lane_hot.astype(jnp.float32), NT, EXACT)
    lanes = iota((n, LANES), 1)
    missed = jnp.max(jnp.where(place >= sum(chunks), 1.0, 0.0), axis=1, keepdims=True)
    keys = jnp.where(lanes < sum(chunks), keys, jnp.where(lanes == LANES - 1, missed, 0.0))
    keys_out[...] = keys.reshape(n, 1, LANES)

    loads[2].wait()
    values = emb_ref[...].astype(jnp.float32)
    unit = (
        values * lax.rsqrt(jnp.sum(values * values, axis=1, keepdims=True) + epsilon)
    ).astype(jnp.bfloat16)

    def pack(piece, turn):
        size = chunks[piece]
        base = quarter_of(turn) * quarter
        local = place - starts[piece]
        slot = jnp.where((local >= 0) & (local < size), (owner - base) * size + local, -1)
        hot = (iota((quarter * size, count), 0) == slot).astype(jnp.bfloat16)
        packed = dot(hot, unit, NN).astype(jnp.bfloat16)
        rows_out[piece][pl.ds(base, quarter)] = packed.reshape(quarter, size, width)

    def send_keys(peer):
        return remote(
            keys_out.at[peer], keys_in.at[me], keys_out_sem, keys_in_sem, peer
        )

    others = pl.ds(0, n - 1)
    next_one = (me + 1) % n

    def take_keys():
        return remote(
            keys_out.at[others], keys_in.at[others], keys_out_sem, keys_in_sem, next_one
        )

    def send_rows(piece, peer):
        return remote(
            rows_out[piece].at[peer], rows_in[piece].at[me],
            rows_out_sem.at[piece], rows_in_sem.at[piece], peer,
        )

    def take_rows(piece):
        return remote(
            rows_out[piece].at[others], rows_in[piece].at[others],
            rows_out_sem.at[piece], rows_in_sem.at[piece], next_one,
        )

    def send_best(peer):
        return remote(
            best_out.at[peer], best_in.at[me], best_out_sem, best_in_sem, peer
        )

    def take_best():
        return remote(
            best_out.at[others], best_in.at[others], best_out_sem, best_in_sem, next_one
        )

    own = [
        pltpu.make_async_copy(rows_out[piece].at[me], rows_in[piece].at[me], own_sem.at[piece])
        for piece in range(pieces)
    ]
    own_keys = pltpu.make_async_copy(keys_out.at[me], keys_in.at[me], own_sem.at[pieces])
    own_best = pltpu.make_async_copy(best_out.at[me], best_in.at[me], own_sem.at[pieces + 1])

    for turn in range(4):
        pack(0, turn)
    pl.semaphore_wait(barrier, n - 1)
    for piece in range(pieces):
        for turn in range(4):
            if piece > 0:
                pack(piece, turn)
            each(lambda peer: send_rows(piece, peer).start(), (turn,))
        own[piece].start()
        if piece == 0:
            each(lambda peer: send_keys(peer).start())
            own_keys.start()

    take_keys().wait_recv()
    own_keys.wait()
    got = keys_in[...].reshape(n, LANES)
    over_ref[0, 0] = jnp.max(jnp.where(lanes == LANES - 1, got, 0.0))
    key_rows, key_columns, floors, spreads, sources = [], [], [], [], []
    for size, start in zip(chunks, starts):
        block = n * size
        source = (iota((n, block), 1) // size == iota((n, block), 0)).astype(jnp.float32)
        spread = iota((LANES, block), 0) == iota((LANES, block), 1) % size + start
        by_lane = dot(got, source, TN, EXACT)
        row = jnp.sum(jnp.where(spread, by_lane, 0.0), axis=0, keepdims=True)
        key_rows.append(row)
        key_columns.append(column(row))
        floors.append(jnp.floor(row * (1.0 / big)) * big)
        spreads.append(spread.astype(jnp.float32))
        sources.append(source)

    best = [jnp.full((1, n * size), -1.0, jnp.float32) for size in chunks]
    for piece, size in enumerate(chunks):
        take_rows(piece).wait_recv()
        own[piece].wait()
        here = rows_in[piece][...].reshape(n * size, width)
        for other in range(piece + 1):
            there = rows_in[other][...].reshape(n * chunks[other], width)
            pairs = [(here, piece, there, other)]
            if other != piece:
                pairs.append((there, other, here, piece))
            for members, m, queries, q in pairs:
                scores = dot(members, queries, NT)
                allowed = (key_columns[m] > floors[q]) & (key_columns[m] < key_rows[q])
                top = jnp.max(jnp.where(allowed, scores, -1.0), axis=0, keepdims=True)
                best[q] = jnp.maximum(best[q], top)
    answer = jnp.zeros((n, LANES), jnp.float32)
    for piece in range(pieces):
        answer = answer + dot(sources[piece] * best[piece], spreads[piece], NT, EXACT)
    best_out[...] = answer.reshape(n, 1, LANES)
    each(lambda peer: send_best(peer).start(), (2, 0, 1, 3))
    own_best.start()

    take_keys().wait_send()
    for piece in range(pieces):
        take_rows(piece).wait_send()
    take_best().wait_recv()
    own_best.wait()
    by_row = dot(best_in[...].reshape(n, LANES), owner_hot.astype(jnp.float32), TN, EXACT)
    out_ref[...] = jnp.sum(jnp.where(lane_hot, by_row, 0.0), axis=0, keepdims=True)
    take_best().wait_send()


def exchange(embeddings, cluster_ids, ranks, chunks, number):
    splits = lax.axis_size("split")
    n = lax.axis_size("loader") * splits
    count, width = embeddings.shape
    big = 1 << (n * count + 1).bit_length()
    dma = pltpu.SemaphoreType.DMA
    vmem = pl.BlockSpec(memory_space=pltpu.VMEM)
    rows = [pltpu.VMEM((n, size, width), jnp.bfloat16) for size in chunks]
    return pl.pallas_call(
        functools.partial(kernel, n, splits, chunks, big),
        out_shape=(
            jax.ShapeDtypeStruct((1, count), jnp.float32),
            jax.ShapeDtypeStruct((1, 1), jnp.float32),
        ),
        in_specs=[pl.BlockSpec(memory_space=pl.ANY)] * 3,
        out_specs=(vmem, pl.BlockSpec(memory_space=pltpu.SMEM)),
        scratch_shapes=[
            *rows,
            *rows,
            *[pltpu.VMEM((n, 1, LANES), jnp.float32)] * 4,
            dma((len(chunks),)),
            dma((len(chunks),)),
            *[dma] * 4,
            dma((len(chunks) + 2,)),
            pltpu.VMEM((count, width), embeddings.dtype),
            pltpu.VMEM((1, count), jnp.int32),
            pltpu.VMEM((1, count), jnp.int32),
            dma((3,)),
        ],
        compiler_params=pltpu.CompilerParams(collective_id=number, has_side_effects=True, vmem_limit_bytes=None if number == 0 else 67_043_328),
    )(embeddings, cluster_ids, ranks)


PLANES = 4
POOL = 20
STRIP = 4
EXTRA = 8


def pooled_kernel(
    n, splits, big, emb_hbm, cid_hbm, rank_hbm, out_ref, over_ref,
    emb_ref, cid_ref, rank_ref, rows_out, rows_in, pool_out, pool_in, extra_out, extra_in,
    meta_out, meta_in, keys_out, keys_in, best_out, best_in,
    load_sem, rows_out_sem, rows_in_sem, pool_sem, meta_sem, extra_sem, keys_sem, best_sem, ready,
):
    me = lax.axis_index("loader") * splits + lax.axis_index("split")
    count, width = emb_hbm.shape
    wide = n // PLANES
    z, j = me // wide, me % wide
    upper = z // 2
    farthest = 3 - 3 * upper
    order = (farthest, farthest - 1 + 2 * upper, 1 - z + 4 * upper, z)
    rows_of = wide // splits
    chip = j // 2

    def position(inner):
        return inner, inner // splits, inner % splits

    def near(turn, core):
        other = chip + turn
        return position(2 * jnp.where(other >= wide // 2, other - wide // 2, other) + core)

    partner = position(j + 1 - 2 * (j % 2))
    column_pair = (position(j), partner)
    around = [near(turn, core) for turn in range(1, wide // 2) for core in range(2)]
    chips = [jnp.where(chip <= k, k + 1, k) for k in reversed(range(wide // 2 - 1))]
    ranked = [position(2 * other + core) for core in range(2) for other in chips]

    def at(plane, spot):
        return plane * wide + spot[0], {"loader": plane * rows_of + spot[1], "split": spot[2]}

    def everyone(act):
        for peer in range(n):
            where = {"loader": peer // splits, "split": peer % splits}
            pl.when(me != peer)(functools.partial(act, peer, where))

    def remote(source, target, send, receive, peer):
        return pltpu.make_async_remote_copy(
            src_ref=source, dst_ref=target, send_sem=send, recv_sem=receive,
            device_id=peer, device_id_type=pl.DeviceIdType.MESH,
        )

    def signal(semaphore, peer):
        pl.semaphore_signal(semaphore, inc=1, device_id=peer, device_id_type=pl.DeviceIdType.MESH)

    barrier = pltpu.get_barrier_semaphore()
    for turn in range(3):
        for spot in column_pair:
            signal(barrier, at(order[turn], spot)[1])
    for spot in (partner, *around):
        signal(barrier, at(z, spot)[1])

    bands = 4
    band = count // bands
    pairs = [(cid_hbm, cid_ref), (rank_hbm, rank_ref)]
    for i in range(bands):
        rows = pl.ds(i * band, band)
        pairs.append((emb_hbm.at[rows], emb_ref.at[rows]))
    loads = [
        pltpu.make_async_copy(source, target, load_sem.at[i])
        for i, (source, target) in enumerate(pairs)
    ]
    for load in (loads[0], *loads[2:], loads[1]):
        load.start()
    earlier = (iota((count, count), 0) < iota((count, count), 1)).astype(jnp.bfloat16)
    loads[0].wait()

    owner = cid_ref[...] % n
    plane = owner // wide
    owner_hot = iota((n, count), 0) == owner
    so_far = dot(owner_hot.astype(jnp.bfloat16), earlier, NN)
    place = jnp.sum(jnp.where(owner_hot, so_far, 0.0), axis=0, keepdims=True).astype(jnp.int32)
    spill = jnp.maximum(so_far - TILE, 0.0)
    pooled = jnp.zeros((1, count), jnp.float32)
    for p in range(PLANES):
        here = jnp.sum(spill[p * wide : (p + 1) * wide], axis=0, keepdims=True)
        pooled = jnp.where(plane == p, here, pooled)
    pooled = pooled.astype(jnp.int32)
    spilled = place >= TILE
    fits = (place < TILE + EXTRA) & (pooled < POOL)
    turned = (z + 2 * PLANES - 1 - plane) % PLANES
    pool_row = jnp.where(spilled & fits, turned * POOL + pooled, -1)
    pool_hot = (iota((LANES, count), 0) == pool_row).astype(jnp.bfloat16)
    units = []
    for i in range(bands):
        loads[2 + i].wait()
        values = emb_ref[i * band : (i + 1) * band].astype(jnp.float32)
        scale = lax.rsqrt(jnp.sum(values * values, axis=1, keepdims=True) + epsilon)
        units.append((values * scale).astype(jnp.bfloat16))
    unit = jnp.concatenate(units, axis=0)
    strips = POOL // STRIP
    pool = dot(pool_hot[: PLANES * POOL], unit, NN).astype(jnp.bfloat16)
    pool_out[...] = pool.reshape(PLANES * strips, STRIP, width)
    own_pool = pl.ds((PLANES - 1) * strips, strips)
    pool_in[own_pool] = pool_out[own_pool]
    slot = jnp.where(spilled, -1, owner * TILE + place)

    def pack(plane):
        size = wide * TILE
        hot = (iota((size, count), 0) + plane * size == slot).astype(jnp.bfloat16)
        packed = dot(hot, unit, NN).astype(jnp.bfloat16)
        rows_out[pl.ds(plane * wide, wide)] = packed.reshape(wide, TILE, width)

    def send_rows(plane, spots):
        for spot in spots:
            peer, where = at(plane, spot)
            remote(
                rows_out.at[peer], rows_in.at[me], rows_out_sem, rows_in_sem.at[z], where
            ).start()

    others = pl.ds(0, n - 1)
    next_one = at(z, partner)[1]
    pools = pl.ds(0, (PLANES - 1) * strips)
    fellows = pl.ds(0, wide - 1)
    take_pools = remote(
        pool_out.at[pools], pool_in.at[pools], pool_sem.at[0], pool_sem.at[1], next_one
    )
    take_meta = remote(
        meta_in.at[pl.ds(0, PLANES - 1)], meta_in.at[pl.ds(0, PLANES - 1)],
        meta_sem.at[0], meta_sem.at[1], next_one,
    )
    take_extra = remote(
        extra_out.at[fellows], extra_in.at[fellows], extra_sem.at[0], extra_sem.at[1], next_one
    )
    take_keys = remote(
        keys_out.at[others], keys_in.at[others], keys_sem.at[0], keys_sem.at[1], next_one
    )
    take_best = remote(
        best_in.at[others], best_in.at[others], best_sem.at[0], best_sem.at[1], next_one
    )
    sent_rows = remote(
        rows_out.at[others], rows_in.at[others], rows_out_sem, rows_in_sem.at[0], next_one
    )

    def take_rows(source, many):
        block = pl.ds(0, many)
        remote(
            rows_out.at[block], rows_in.at[block], rows_out_sem, rows_in_sem.at[source], next_one
        ).wait_recv()

    def send_pool(plane):
        step = (z + 2 * PLANES - 1 - plane) % PLANES
        block = pl.ds(step * strips, strips)
        where = at(plane, column_pair[0])[1]
        remote(
            pool_out.at[block], pool_in.at[block], pool_sem.at[0], pool_sem.at[1], where
        ).start()

    def send_meta(plane):
        step = (z + 2 * PLANES - 1 - plane) % PLANES
        where = at(plane, column_pair[0])[1]
        remote(meta_out, meta_in.at[step], meta_sem.at[0], meta_sem.at[1], where).start()

    pl.semaphore_wait(barrier, 2 * (PLANES - 1) + wide - 1)
    for turn in range(3):
        send_pool(order[turn])
    for spot in around:
        signal(ready, at(z, spot)[1])
    code = ((owner % wide) * EXTRA + place - TILE + 1).astype(jnp.float32)
    code = jnp.broadcast_to(jnp.where(spilled, code, 0.0), (8, count)).astype(jnp.bfloat16)
    meta_out[...] = dot(code, pool_hot, NT)[:1]
    meta_in[PLANES - 1] = meta_out[...]
    for turn in range(3):
        send_meta(order[turn])
    for turn in range(3):
        pack(order[turn])
        send_rows(order[turn], column_pair)
    pack(z)
    rows_in[me] = rows_out[me]
    send_rows(z, [partner, *around])
    loads[1].wait()
    lanes = iota((n, LANES), 1)
    lane_hot = iota((LANES, count), 0) == place
    key = ((cid_ref[...] // n) * big + rank_ref[...] + 1).astype(jnp.float32)
    keys = dot(jnp.where(owner_hot, key, 0.0), lane_hot.astype(jnp.float32), NT, EXACT)
    missed = jnp.max(jnp.where(spilled & ~fits, 1.0, 0.0), axis=1, keepdims=True)
    keys = jnp.where(lanes < TILE + EXTRA, keys, jnp.where(lanes == LANES - 1, missed, 0.0))
    keys_out[...] = keys.reshape(n, 1, LANES)
    pl.semaphore_wait(ready, wide - 2)

    def send_keys(peer, where):
        remote(
            keys_out.at[peer], keys_in.at[me], keys_sem.at[0], keys_sem.at[1], where
        ).start()

    everyone(send_keys)
    keys_in[me] = keys_out[me]

    take_meta.wait_recv()
    segment = iota((1, LANES), 1) // POOL
    codes = jnp.full((1, LANES), -1.0, jnp.float32)
    for step in range(PLANES):
        got = meta_in[step]
        codes = jnp.where((segment == step) & (got > 0.0), got + step * 128.0, codes)
    codes = codes[:, : PLANES * POOL]
    block = wide * PLANES * EXTRA
    shape = (block, PLANES * POOL)
    line = iota(shape, 0)
    wanted = (line // EXTRA % PLANES) * 128 + line // (PLANES * EXTRA) * EXTRA + line % EXTRA + 1
    expand = (wanted.astype(jnp.float32) == codes).astype(jnp.bfloat16)
    take_pools.wait_recv()
    send_rows(order[0], around)
    expanded = dot(expand, pool_in[...].reshape(PLANES * POOL, width), NN).astype(jnp.bfloat16)
    extra_out[...] = expanded.reshape(wide, PLANES * EXTRA, width)
    extra_in[j] = extra_out[j]

    for spot in (partner, *around):
        remote(
            extra_out.at[spot[0]], extra_in.at[j], extra_sem.at[0], extra_sem.at[1],
            at(z, spot)[1],
        ).start()
    send_rows(order[1], ranked)
    send_rows(order[2], around)

    take_keys.wait_recv()
    over_ref[0, 0] = jnp.max(jnp.where(lanes == LANES - 1, keys_in[...].reshape(n, LANES), 0.0))
    row = iota((wide, LANES), 0)

    def keys_of(source):
        return keys_in[pl.ds(source * wide, wide)].reshape(wide, LANES)

    def plane_keys(source):
        spread = pltpu.roll(keys_of(source), 0, 1, stride=TILE, stride_axis=0)
        mine = iota((wide, LANES), 1) // TILE == row
        return jnp.sum(jnp.where(mine, spread, 0.0), axis=0, keepdims=True)

    run = PLANES * EXTRA
    per_tile = LANES // run
    lane = iota((wide, LANES), 1)
    run_keys = jnp.zeros((wide, LANES), jnp.float32)
    for step in range(PLANES):
        got = keys_of((z + 1 + step) % PLANES)
        moved = pltpu.roll(got, (step * EXTRA - TILE) % LANES, 1)
        run_keys = jnp.where(lane // EXTRA == step, moved, run_keys)
    repeated = run_keys
    for turn in range(1, per_tile):
        repeated = repeated + pltpu.roll(run_keys, turn * run, 1)
    repeated = jnp.where(lane // run == row % per_tile, repeated, 0.0)
    halves = [
        jnp.sum(repeated[first : first + per_tile], axis=0, keepdims=True)
        for first in range(0, wide, per_tile)
    ]

    def keyed(line):
        return line, column(line), jnp.floor(line * (1.0 / big)) * big

    sources = (order[3], None, order[2], order[0], order[1])
    keyring, best = [], []
    for source in sources:
        if source is None:
            line = jnp.concatenate(halves, axis=1)
        else:
            line = plane_keys(source)
        keyring.append(keyed(line))
        best.append(jnp.full(line.shape, -1.0, jnp.float32))

    def fetch(index):
        if sources[index] is None:
            return extra_in[...].reshape(block, width)
        return rows_in[pl.ds(sources[index] * wide, wide)].reshape(wide * TILE, width)

    def score(members, m, queries, q):
        scores = dot(members, queries, NT)
        key_row, _, floor = keyring[q]
        key_column = keyring[m][1]
        allowed = (key_column > floor) & (key_column < key_row)
        top = jnp.max(jnp.where(allowed, scores, -1.0), axis=0, keepdims=True)
        best[q] = jnp.maximum(best[q], top)

    def arrive(index):
        if sources[index] is None:
            take_extra.wait_recv()
        else:
            take_rows(sources[index], wide - 1 if index == 0 else wide)

    def answer(index):
        plane = sources[index]
        for half in range(tiles):
            best_out[plane * tiles + half, 0:1] = best[index]
            best_out[plane * tiles + half, 1:2] = best[1][:, half * LANES : (half + 1) * LANES]

        def send_best(inner):
            peer, where = at(plane, (inner, inner // splits, inner % splits))
            remote(
                best_out.at[plane * tiles + inner // per_tile], best_in.at[me],
                best_sem.at[0], best_sem.at[1], where,
            ).start()

        for inner in range(wide):
            if index == 0:
                pl.when(j != inner)(functools.partial(send_best, inner))
            else:
                send_best(inner)

    tiles = wide // per_tile
    last = len(sources) - 1
    for index in range(last):
        arrive(index)
        new = fetch(index)
        for other in range(index):
            old = fetch(other)
            if index < 3 or other > 0:
                score(new, index, old, other)
            score(old, other, new, index)
        score(new, index, new, index)
    arrive(last)
    new = fetch(last)
    for other in (1, 3, 2, 0):
        if other == 0:
            score(fetch(3), 3, fetch(0), 0)
        score(new, last, fetch(other), other)
        if other != 1:
            answer(other)
    for other in range(last):
        score(fetch(other), other, new, last)
    score(new, last, new, last)
    answer(last)
    best_in[me] = best_out[z * tiles + j // per_tile]

    take_best.wait_recv()
    answers = pltpu.roll(best_in[:, 0, :], (LANES - j * TILE) % LANES, 1)
    spare = best_in[:, 1, :]
    shifted = []
    for p in range(PLANES):
        step = (z + 2 * PLANES - 1 - p) % PLANES
        begin = j % per_tile * PLANES * EXTRA + step * EXTRA
        shifted.append(
            pltpu.roll(spare[p * wide : (p + 1) * wide], (LANES + TILE - begin) % LANES, 1)
        )
    table = jnp.where(lanes < TILE, answers, jnp.concatenate(shifted, axis=0))
    kept = 2 * TILE
    by_row = dot(table[:, :kept], owner_hot.astype(jnp.float32), TN, EXACT)
    out_ref[...] = jnp.sum(jnp.where(lane_hot[:kept], by_row, 0.0), axis=0, keepdims=True)
    take_pools.wait_send()
    for step in range(PLANES - 1):
        remote(meta_out, meta_in.at[step], meta_sem.at[0], meta_sem.at[1], next_one).wait_send()
    take_keys.wait_send()
    take_extra.wait_send()
    sent_rows.wait_send()
    take_best.wait_send()


def pooled_exchange(embeddings, cluster_ids, ranks):
    splits = lax.axis_size("split")
    n = lax.axis_size("loader") * splits
    count, width = embeddings.shape
    big = 1 << (n * count + 1).bit_length()
    wide = n // PLANES
    dma = pltpu.SemaphoreType.DMA

    def held(*shape):
        return pltpu.VMEM(shape, jnp.bfloat16)

    def told(*shape):
        return pltpu.VMEM(shape, jnp.float32)

    return pl.pallas_call(
        functools.partial(pooled_kernel, n, splits, big),
        out_shape=(
            jax.ShapeDtypeStruct((1, count), jnp.float32),
            jax.ShapeDtypeStruct((1, 1), jnp.float32),
        ),
        in_specs=[pl.BlockSpec(memory_space=pl.ANY)] * 3,
        out_specs=(
            pl.BlockSpec(memory_space=pltpu.VMEM), pl.BlockSpec(memory_space=pltpu.SMEM)
        ),
        scratch_shapes=[
            pltpu.VMEM((count, width), embeddings.dtype),
            pltpu.VMEM((1, count), jnp.int32),
            pltpu.VMEM((1, count), jnp.int32),
            *[held(n, TILE, width)] * 2,
            *[held(PLANES * POOL // STRIP, STRIP, width)] * 2,
            *[held(wide, PLANES * EXTRA, width)] * 2,
            told(1, LANES),
            told(PLANES, 1, LANES),
            *[told(n, 1, LANES)] * 2,
            told(PLANES * (wide * PLANES * EXTRA // LANES), 2, LANES),
            told(n, 2, LANES),
            dma((6,)),
            dma,
            dma((PLANES,)),
            *[dma((2,))] * 5,
            pltpu.SemaphoreType.REGULAR,
        ],
        compiler_params=pltpu.CompilerParams(collective_id=0, has_side_effects=True),
    )(embeddings, cluster_ids, ranks)


def two_sizes(embeddings, cluster_ids, ranks):
    n = lax.axis_size("loader") * lax.axis_size("split")
    count = embeddings.shape[0]
    cluster_ids, ranks = cluster_ids.reshape(1, count), ranks.reshape(1, count)
    most = CLUSTERS // n * CAP
    small, over = pooled_exchange(embeddings, cluster_ids, ranks)
    out = lax.cond(
        over[0, 0] > 0.0,
        lambda: exchange(embeddings, cluster_ids, ranks, (TILE, most - TILE), 1)[0],
        lambda: small,
    )
    return out.reshape(count)


def tile_scores(queries, remote):
    return jnp.einsum("kqd,kmd->kqm", queries, remote, preferred_element_type=jnp.float32)


def row_maxima(scores, query_rank, member_rank):
    allowed = (member_rank[:, None, :] >= 0) & (member_rank[:, None, :] < query_rank[:, :, None])
    return jnp.max(jnp.where(allowed, scores, jnp.float32(-1.0)), axis=2)


def small_tiles(embeddings, cluster_ids, ranks):
    loader_count = lax.axis_size("loader")
    split_count = lax.axis_size("split")
    rows_here = embeddings.shape[0]
    width = embeddings.shape[1]
    values = embeddings.astype(jnp.float32)
    unit = (values * lax.rsqrt(jnp.sum(values * values, axis=1, keepdims=True) + epsilon)).astype(
        jnp.bfloat16
    )
    cluster = cluster_ids[:, 0]
    row_index = jnp.arange(rows_here, dtype=jnp.int32)
    same_cluster = cluster[:, None] == cluster[None, :]
    earlier = row_index[None, :] < row_index[:, None]
    position = jnp.sum((same_cluster & earlier).astype(jnp.int32), axis=1)
    slot_count = CLUSTERS * CAP
    device_count = loader_count * split_count
    owner_flat = cluster % device_count
    cluster_slot = cluster // device_count
    owned = CLUSTERS // device_count
    target = (
        (cluster_slot * loader_count + owner_flat // split_count) * split_count
        + owner_flat % split_count
    ) * CAP + position
    send_rows = (
        jnp.zeros((slot_count, width), jnp.bfloat16)
        .at[target]
        .set(unit)
        .reshape(owned, loader_count, split_count, CAP, width)
    )
    send_rank = (
        jnp.full((slot_count,), -1, jnp.int32)
        .at[target]
        .set(ranks)
        .reshape(owned, loader_count, split_count, CAP)
    )

    def swap(block):
        return lax.all_to_all(
            lax.all_to_all(block, "loader", split_axis=1, concat_axis=1, tiled=True),
            "split",
            split_axis=2,
            concat_axis=2,
            tiled=True,
        )

    members = swap(send_rows).reshape(owned, -1, width)
    member_rank = swap(send_rank).reshape(owned, -1)
    best = row_maxima(tile_scores(members, members), member_rank, member_rank)
    returned = swap(best.reshape(owned, loader_count, split_count, CAP))
    return returned.reshape(-1)[target]


def shards(embeddings, cluster_ids, ranks):
    n = lax.axis_size("loader") * lax.axis_size("split")
    fits = n % 4 == 0 and CLUSTERS // n * CAP == 2 * TILE
    fits = fits and n // PLANES % lax.axis_size("split") == 0
    return (two_sizes if fits else small_tiles)(embeddings, cluster_ids, ranks)


def solution(mesh):
    return jax.shard_map(
        shards,
        mesh=mesh,
        in_specs=(
            P(("loader", "split"), None),
            P(("loader", "split"), None),
            P(("loader", "split")),
        ),
        out_specs=P(("loader", "split")),
        check_vma=False,
    )
```

```python
import functools

import jax
import jax.numpy as jnp
from jax import lax
from jax.experimental import pallas as pl
from jax.experimental.pallas import tpu as pltpu
from jax.sharding import PartitionSpec as P

CLUSTERS = 256
CAP = 4
LANES = 128
TILE = 16

epsilon = 1e-06
EXACT = lax.Precision.HIGHEST
NN = (((1,), (0,)), ((), ()))
NT = (((1,), (1,)), ((), ()))
TN = (((0,), (0,)), ((), ()))
QUARTERS = (2, 1, 3, 0)


def dot(a, b, dims, precision=None):
    return lax.dot_general(a, b, dims, precision=precision, preferred_element_type=jnp.float32)


def iota(shape, axis):
    return lax.broadcasted_iota(jnp.int32, shape, axis)


def column(row):
    return jnp.transpose(jnp.broadcast_to(row, (LANES, row.shape[1])))[:, :1]


def kernel(n, splits, chunks, big, emb_hbm, cid_hbm, rank_hbm, out_ref, over_ref, *scratch):
    pieces = len(chunks)
    rows_out, rows_in = scratch[:pieces], scratch[pieces : 2 * pieces]
    (
        keys_out, keys_in, best_out, best_in,
        rows_out_sem, rows_in_sem, keys_out_sem, keys_in_sem, best_out_sem, best_in_sem, own_sem,
        emb_ref, cid_ref, rank_ref, load_sem,
    ) = scratch[2 * pieces :]
    me = lax.axis_index("loader") * splits + lax.axis_index("split")
    count, width = emb_hbm.shape
    quarter = n // 4
    mine, inner = me // quarter, me % quarter
    sign = 1 - 2 * (mine // 2)
    starts = [sum(chunks[:i]) for i in range(pieces)]

    def where_is(index):
        return {"loader": index // splits, "split": index % splits}

    def quarter_of(turn):
        return (mine + sign * QUARTERS[turn] + 4) % 4

    def each(act, turns=range(4)):
        for turn in turns:
            base = quarter_of(turn) * quarter
            first = 1 if QUARTERS[turn] == 0 else 0

            def step(i, carry):
                act(base + (inner + i) % quarter)
                return carry

            lax.fori_loop(first, quarter, step, 0)

    def remote(source, target, send, receive, peer):
        return pltpu.make_async_remote_copy(
            src_ref=source, dst_ref=target, send_sem=send, recv_sem=receive,
            device_id=where_is(peer), device_id_type=pl.DeviceIdType.MESH,
        )

    barrier = pltpu.get_barrier_semaphore()
    each(
        lambda peer: pl.semaphore_signal(
            barrier, inc=1, device_id=where_is(peer), device_id_type=pl.DeviceIdType.MESH
        )
    )

    loads = [
        pltpu.make_async_copy(source, target, load_sem.at[i])
        for i, (source, target) in enumerate(
            ((cid_hbm, cid_ref), (rank_hbm, rank_ref), (emb_hbm, emb_ref))
        )
    ]
    for load in loads:
        load.start()
    loads[0].wait()

    owner = cid_ref[...] % n
    before = (column(owner) == owner) & (iota((count, count), 0) < iota((count, count), 1))
    place = jnp.sum(before.astype(jnp.int32), axis=0, keepdims=True)
    owner_hot = iota((n, count), 0) == owner
    lane_hot = iota((LANES, count), 0) == place

    loads[1].wait()
    key = ((cid_ref[...] // n) * big + rank_ref[...] + 1).astype(jnp.float32)
    keys = dot(jnp.where(owner_hot, key, 0.0), lane_hot.astype(jnp.float32), NT, EXACT)
    lanes = iota((n, LANES), 1)
    missed = jnp.max(jnp.where(place >= sum(chunks), 1.0, 0.0), axis=1, keepdims=True)
    keys = jnp.where(lanes < sum(chunks), keys, jnp.where(lanes == LANES - 1, missed, 0.0))
    keys_out[...] = keys.reshape(n, 1, LANES)

    loads[2].wait()
    values = emb_ref[...].astype(jnp.float32)
    unit = (
        values * lax.rsqrt(jnp.sum(values * values, axis=1, keepdims=True) + epsilon)
    ).astype(jnp.bfloat16)

    def pack(piece, turn):
        size = chunks[piece]
        base = quarter_of(turn) * quarter
        local = place - starts[piece]
        slot = jnp.where((local >= 0) & (local < size), (owner - base) * size + local, -1)
        hot = (iota((quarter * size, count), 0) == slot).astype(jnp.bfloat16)
        packed = dot(hot, unit, NN).astype(jnp.bfloat16)
        rows_out[piece][pl.ds(base, quarter)] = packed.reshape(quarter, size, width)

    def send_keys(peer):
        return remote(
            keys_out.at[peer], keys_in.at[me], keys_out_sem, keys_in_sem, peer
        )

    others = pl.ds(0, n - 1)
    next_one = (me + 1) % n

    def take_keys():
        return remote(
            keys_out.at[others], keys_in.at[others], keys_out_sem, keys_in_sem, next_one
        )

    def send_rows(piece, peer):
        return remote(
            rows_out[piece].at[peer], rows_in[piece].at[me],
            rows_out_sem.at[piece], rows_in_sem.at[piece], peer,
        )

    def take_rows(piece):
        return remote(
            rows_out[piece].at[others], rows_in[piece].at[others],
            rows_out_sem.at[piece], rows_in_sem.at[piece], next_one,
        )

    def send_best(peer):
        return remote(
            best_out.at[peer], best_in.at[me], best_out_sem, best_in_sem, peer
        )

    def take_best():
        return remote(
            best_out.at[others], best_in.at[others], best_out_sem, best_in_sem, next_one
        )

    own = [
        pltpu.make_async_copy(rows_out[piece].at[me], rows_in[piece].at[me], own_sem.at[piece])
        for piece in range(pieces)
    ]
    own_keys = pltpu.make_async_copy(keys_out.at[me], keys_in.at[me], own_sem.at[pieces])
    own_best = pltpu.make_async_copy(best_out.at[me], best_in.at[me], own_sem.at[pieces + 1])

    for turn in range(4):
        pack(0, turn)
    pl.semaphore_wait(barrier, n - 1)
    for piece in range(pieces):
        for turn in range(4):
            if piece > 0:
                pack(piece, turn)
            each(lambda peer: send_rows(piece, peer).start(), (turn,))
        own[piece].start()
        if piece == 0:
            each(lambda peer: send_keys(peer).start())
            own_keys.start()

    take_keys().wait_recv()
    own_keys.wait()
    got = keys_in[...].reshape(n, LANES)
    over_ref[0, 0] = jnp.max(jnp.where(lanes == LANES - 1, got, 0.0))
    key_rows, key_columns, floors, spreads, sources = [], [], [], [], []
    for size, start in zip(chunks, starts):
        block = n * size
        source = (iota((n, block), 1) // size == iota((n, block), 0)).astype(jnp.float32)
        spread = iota((LANES, block), 0) == iota((LANES, block), 1) % size + start
        by_lane = dot(got, source, TN, EXACT)
        row = jnp.sum(jnp.where(spread, by_lane, 0.0), axis=0, keepdims=True)
        key_rows.append(row)
        key_columns.append(column(row))
        floors.append(jnp.floor(row * (1.0 / big)) * big)
        spreads.append(spread.astype(jnp.float32))
        sources.append(source)

    best = [jnp.full((1, n * size), -1.0, jnp.float32) for size in chunks]
    for piece, size in enumerate(chunks):
        take_rows(piece).wait_recv()
        own[piece].wait()
        here = rows_in[piece][...].reshape(n * size, width)
        for other in range(piece + 1):
            there = rows_in[other][...].reshape(n * chunks[other], width)
            pairs = [(here, piece, there, other)]
            if other != piece:
                pairs.append((there, other, here, piece))
            for members, m, queries, q in pairs:
                scores = dot(members, queries, NT)
                allowed = (key_columns[m] > floors[q]) & (key_columns[m] < key_rows[q])
                top = jnp.max(jnp.where(allowed, scores, -1.0), axis=0, keepdims=True)
                best[q] = jnp.maximum(best[q], top)
    answer = jnp.zeros((n, LANES), jnp.float32)
    for piece in range(pieces):
        answer = answer + dot(sources[piece] * best[piece], spreads[piece], NT, EXACT)
    best_out[...] = answer.reshape(n, 1, LANES)
    each(lambda peer: send_best(peer).start(), (2, 0, 1, 3))
    own_best.start()

    take_keys().wait_send()
    for piece in range(pieces):
        take_rows(piece).wait_send()
    take_best().wait_recv()
    own_best.wait()
    by_row = dot(best_in[...].reshape(n, LANES), owner_hot.astype(jnp.float32), TN, EXACT)
    out_ref[...] = jnp.sum(jnp.where(lane_hot, by_row, 0.0), axis=0, keepdims=True)
    take_best().wait_send()


def exchange(embeddings, cluster_ids, ranks, chunks, number):
    splits = lax.axis_size("split")
    n = lax.axis_size("loader") * splits
    count, width = embeddings.shape
    big = 1 << (n * count + 1).bit_length()
    dma = pltpu.SemaphoreType.DMA
    vmem = pl.BlockSpec(memory_space=pltpu.VMEM)
    rows = [pltpu.VMEM((n, size, width), jnp.bfloat16) for size in chunks]
    return pl.pallas_call(
        functools.partial(kernel, n, splits, chunks, big),
        out_shape=(
            jax.ShapeDtypeStruct((1, count), jnp.float32),
            jax.ShapeDtypeStruct((1, 1), jnp.float32),
        ),
        in_specs=[pl.BlockSpec(memory_space=pl.ANY)] * 3,
        out_specs=(vmem, pl.BlockSpec(memory_space=pltpu.SMEM)),
        scratch_shapes=[
            *rows,
            *rows,
            *[pltpu.VMEM((n, 1, LANES), jnp.float32)] * 4,
            dma((len(chunks),)),
            dma((len(chunks),)),
            *[dma] * 4,
            dma((len(chunks) + 2,)),
            pltpu.VMEM((count, width), embeddings.dtype),
            pltpu.VMEM((1, count), jnp.int32),
            pltpu.VMEM((1, count), jnp.int32),
            dma((3,)),
        ],
        compiler_params=pltpu.CompilerParams(collective_id=number, has_side_effects=True, vmem_limit_bytes=None if number == 0 else 67_043_328),
    )(embeddings, cluster_ids, ranks)


PLANES = 4
POOL = 20
STRIP = 4
EXTRA = 8


def pooled_kernel(
    n, splits, big, emb_hbm, cid_hbm, rank_hbm, out_ref, over_ref,
    emb_ref, cid_ref, rank_ref, rows_out, rows_in, pool_out, pool_in, extra_out, extra_in,
    meta_out, meta_in, keys_out, keys_in, best_out, best_in,
    load_sem, rows_out_sem, rows_in_sem, pool_sem, meta_sem, extra_sem, keys_sem, best_sem, ready,
):
    me = lax.axis_index("loader") * splits + lax.axis_index("split")
    count, width = emb_hbm.shape
    wide = n // PLANES
    z, j = me // wide, me % wide
    upper = z // 2
    farthest = 3 - 3 * upper
    order = (farthest, farthest - 1 + 2 * upper, 1 - z + 4 * upper, z)
    rows_of = wide // splits
    chip = j // 2

    def position(inner):
        return inner, inner // splits, inner % splits

    def near(turn, core):
        other = chip + turn
        return position(2 * jnp.where(other >= wide // 2, other - wide // 2, other) + core)

    partner = position(j + 1 - 2 * (j % 2))
    column_pair = (position(j), partner)
    around = [near(turn, core) for turn in range(1, wide // 2) for core in range(2)]
    chips = [jnp.where(chip <= k, k + 1, k) for k in reversed(range(wide // 2 - 1))]
    ranked = [position(2 * other + core) for core in range(2) for other in chips]

    def at(plane, spot):
        return plane * wide + spot[0], {"loader": plane * rows_of + spot[1], "split": spot[2]}

    def everyone(act):
        for peer in range(n):
            where = {"loader": peer // splits, "split": peer % splits}
            pl.when(me != peer)(functools.partial(act, peer, where))

    def remote(source, target, send, receive, peer):
        return pltpu.make_async_remote_copy(
            src_ref=source, dst_ref=target, send_sem=send, recv_sem=receive,
            device_id=peer, device_id_type=pl.DeviceIdType.MESH,
        )

    def signal(semaphore, peer):
        pl.semaphore_signal(semaphore, inc=1, device_id=peer, device_id_type=pl.DeviceIdType.MESH)

    barrier = pltpu.get_barrier_semaphore()
    for turn in range(3):
        for spot in column_pair:
            signal(barrier, at(order[turn], spot)[1])
    for spot in (partner, *around):
        signal(barrier, at(z, spot)[1])

    bands = 4
    band = count // bands
    pairs = [(cid_hbm, cid_ref), (rank_hbm, rank_ref)]
    for i in range(bands):
        rows = pl.ds(i * band, band)
        pairs.append((emb_hbm.at[rows], emb_ref.at[rows]))
    loads = [
        pltpu.make_async_copy(source, target, load_sem.at[i])
        for i, (source, target) in enumerate(pairs)
    ]
    for load in (loads[0], *loads[2:], loads[1]):
        load.start()
    earlier = (iota((count, count), 0) < iota((count, count), 1)).astype(jnp.bfloat16)
    loads[0].wait()

    owner = cid_ref[...] % n
    plane = owner // wide
    owner_hot = iota((n, count), 0) == owner
    so_far = dot(owner_hot.astype(jnp.bfloat16), earlier, NN)
    place = jnp.sum(jnp.where(owner_hot, so_far, 0.0), axis=0, keepdims=True).astype(jnp.int32)
    spill = jnp.maximum(so_far - TILE, 0.0)
    pooled = jnp.zeros((1, count), jnp.float32)
    for p in range(PLANES):
        here = jnp.sum(spill[p * wide : (p + 1) * wide], axis=0, keepdims=True)
        pooled = jnp.where(plane == p, here, pooled)
    pooled = pooled.astype(jnp.int32)
    spilled = place >= TILE
    fits = (place < TILE + EXTRA) & (pooled < POOL)
    turned = (z + 2 * PLANES - 1 - plane) % PLANES
    pool_row = jnp.where(spilled & fits, turned * POOL + pooled, -1)
    pool_hot = (iota((LANES, count), 0) == pool_row).astype(jnp.bfloat16)
    units = []
    for i in range(bands):
        loads[2 + i].wait()
        values = emb_ref[i * band : (i + 1) * band].astype(jnp.float32)
        scale = lax.rsqrt(jnp.sum(values * values, axis=1, keepdims=True) + epsilon)
        units.append((values * scale).astype(jnp.bfloat16))
    unit = jnp.concatenate(units, axis=0)
    strips = POOL // STRIP
    pool = dot(pool_hot[: PLANES * POOL], unit, NN).astype(jnp.bfloat16)
    pool_out[...] = pool.reshape(PLANES * strips, STRIP, width)
    own_pool = pl.ds((PLANES - 1) * strips, strips)
    pool_in[own_pool] = pool_out[own_pool]
    slot = jnp.where(spilled, -1, owner * TILE + place)

    def pack(plane):
        size = wide * TILE
        hot = (iota((size, count), 0) + plane * size == slot).astype(jnp.bfloat16)
        packed = dot(hot, unit, NN).astype(jnp.bfloat16)
        rows_out[pl.ds(plane * wide, wide)] = packed.reshape(wide, TILE, width)

    def send_rows(plane, spots):
        for spot in spots:
            peer, where = at(plane, spot)
            remote(
                rows_out.at[peer], rows_in.at[me], rows_out_sem, rows_in_sem.at[z], where
            ).start()

    others = pl.ds(0, n - 1)
    next_one = at(z, partner)[1]
    pools = pl.ds(0, (PLANES - 1) * strips)
    fellows = pl.ds(0, wide - 1)
    take_pools = remote(
        pool_out.at[pools], pool_in.at[pools], pool_sem.at[0], pool_sem.at[1], next_one
    )
    take_meta = remote(
        meta_in.at[pl.ds(0, PLANES - 1)], meta_in.at[pl.ds(0, PLANES - 1)],
        meta_sem.at[0], meta_sem.at[1], next_one,
    )
    take_extra = remote(
        extra_out.at[fellows], extra_in.at[fellows], extra_sem.at[0], extra_sem.at[1], next_one
    )
    take_keys = remote(
        keys_out.at[others], keys_in.at[others], keys_sem.at[0], keys_sem.at[1], next_one
    )
    take_best = remote(
        best_in.at[others], best_in.at[others], best_sem.at[0], best_sem.at[1], next_one
    )
    sent_rows = remote(
        rows_out.at[others], rows_in.at[others], rows_out_sem, rows_in_sem.at[0], next_one
    )

    def take_rows(source, many):
        block = pl.ds(0, many)
        remote(
            rows_out.at[block], rows_in.at[block], rows_out_sem, rows_in_sem.at[source], next_one
        ).wait_recv()

    def send_pool(plane):
        step = (z + 2 * PLANES - 1 - plane) % PLANES
        block = pl.ds(step * strips, strips)
        where = at(plane, column_pair[0])[1]
        remote(
            pool_out.at[block], pool_in.at[block], pool_sem.at[0], pool_sem.at[1], where
        ).start()

    def send_meta(plane):
        step = (z + 2 * PLANES - 1 - plane) % PLANES
        where = at(plane, column_pair[0])[1]
        remote(meta_out, meta_in.at[step], meta_sem.at[0], meta_sem.at[1], where).start()

    pl.semaphore_wait(barrier, 2 * (PLANES - 1) + wide - 1)
    for turn in range(3):
        send_pool(order[turn])
    for spot in around:
        signal(ready, at(z, spot)[1])
    code = ((owner % wide) * EXTRA + place - TILE + 1).astype(jnp.float32)
    code = jnp.broadcast_to(jnp.where(spilled, code, 0.0), (8, count)).astype(jnp.bfloat16)
    meta_out[...] = dot(code, pool_hot, NT)[:1]
    meta_in[PLANES - 1] = meta_out[...]
    for turn in range(3):
        send_meta(order[turn])
    for turn in range(3):
        pack(order[turn])
        send_rows(order[turn], column_pair)
    pack(z)
    rows_in[me] = rows_out[me]
    send_rows(z, [partner, *around])
    loads[1].wait()
    lanes = iota((n, LANES), 1)
    lane_hot = iota((LANES, count), 0) == place
    key = ((cid_ref[...] // n) * big + rank_ref[...] + 1).astype(jnp.float32)
    keys = dot(jnp.where(owner_hot, key, 0.0), lane_hot.astype(jnp.float32), NT, EXACT)
    missed = jnp.max(jnp.where(spilled & ~fits, 1.0, 0.0), axis=1, keepdims=True)
    keys = jnp.where(lanes < TILE + EXTRA, keys, jnp.where(lanes == LANES - 1, missed, 0.0))
    keys_out[...] = keys.reshape(n, 1, LANES)
    pl.semaphore_wait(ready, wide - 2)

    def send_keys(peer, where):
        remote(
            keys_out.at[peer], keys_in.at[me], keys_sem.at[0], keys_sem.at[1], where
        ).start()

    everyone(send_keys)
    keys_in[me] = keys_out[me]

    take_meta.wait_recv()
    segment = iota((1, LANES), 1) // POOL
    codes = jnp.full((1, LANES), -1.0, jnp.float32)
    for step in range(PLANES):
        got = meta_in[step]
        codes = jnp.where((segment == step) & (got > 0.0), got + step * 128.0, codes)
    codes = codes[:, : PLANES * POOL]
    block = wide * PLANES * EXTRA
    shape = (block, PLANES * POOL)
    line = iota(shape, 0)
    wanted = (line // EXTRA % PLANES) * 128 + line // (PLANES * EXTRA) * EXTRA + line % EXTRA + 1
    expand = (wanted.astype(jnp.float32) == codes).astype(jnp.bfloat16)
    take_pools.wait_recv()
    send_rows(order[0], around)
    send_rows(order[1], ranked[:5])
    expanded = dot(expand, pool_in[...].reshape(PLANES * POOL, width), NN).astype(jnp.bfloat16)
    extra_out[...] = expanded.reshape(wide, PLANES * EXTRA, width)
    extra_in[j] = extra_out[j]

    for spot in (partner, *around):
        remote(
            extra_out.at[spot[0]], extra_in.at[j], extra_sem.at[0], extra_sem.at[1],
            at(z, spot)[1],
        ).start()
    send_rows(order[2], around)
    send_rows(order[1], ranked[5:])

    take_keys.wait_recv()
    over_ref[0, 0] = jnp.max(jnp.where(lanes == LANES - 1, keys_in[...].reshape(n, LANES), 0.0))
    row = iota((wide, LANES), 0)

    def keys_of(source):
        return keys_in[pl.ds(source * wide, wide)].reshape(wide, LANES)

    def plane_keys(source):
        spread = pltpu.roll(keys_of(source), 0, 1, stride=TILE, stride_axis=0)
        mine = iota((wide, LANES), 1) // TILE == row
        return jnp.sum(jnp.where(mine, spread, 0.0), axis=0, keepdims=True)

    run = PLANES * EXTRA
    per_tile = LANES // run
    lane = iota((wide, LANES), 1)
    run_keys = jnp.zeros((wide, LANES), jnp.float32)
    for step in range(PLANES):
        got = keys_of((z + 1 + step) % PLANES)
        moved = pltpu.roll(got, (step * EXTRA - TILE) % LANES, 1)
        run_keys = jnp.where(lane // EXTRA == step, moved, run_keys)
    repeated = run_keys
    for turn in range(1, per_tile):
        repeated = repeated + pltpu.roll(run_keys, turn * run, 1)
    repeated = jnp.where(lane // run == row % per_tile, repeated, 0.0)
    halves = [
        jnp.sum(repeated[first : first + per_tile], axis=0, keepdims=True)
        for first in range(0, wide, per_tile)
    ]

    def keyed(line):
        return line, column(line), jnp.floor(line * (1.0 / big)) * big

    sources = (order[3], None, order[2], order[0], order[1])
    keyring, best = [], []
    for source in sources:
        if source is None:
            line = jnp.concatenate(halves, axis=1)
        else:
            line = plane_keys(source)
        keyring.append(keyed(line))
        best.append(jnp.full(line.shape, -1.0, jnp.float32))

    def fetch(index):
        if sources[index] is None:
            return extra_in[...].reshape(block, width)
        return rows_in[pl.ds(sources[index] * wide, wide)].reshape(wide * TILE, width)

    def score(members, m, queries, q):
        scores = dot(members, queries, NT)
        key_row, _, floor = keyring[q]
        key_column = keyring[m][1]
        allowed = (key_column > floor) & (key_column < key_row)
        top = jnp.max(jnp.where(allowed, scores, -1.0), axis=0, keepdims=True)
        best[q] = jnp.maximum(best[q], top)

    def arrive(index):
        if sources[index] is None:
            take_extra.wait_recv()
        else:
            take_rows(sources[index], wide - 1 if index == 0 else wide)

    def answer(index):
        plane = sources[index]
        for half in range(tiles):
            best_out[plane * tiles + half, 0:1] = best[index]
            best_out[plane * tiles + half, 1:2] = best[1][:, half * LANES : (half + 1) * LANES]

        def send_best(inner):
            peer, where = at(plane, (inner, inner // splits, inner % splits))
            remote(
                best_out.at[plane * tiles + inner // per_tile], best_in.at[me],
                best_sem.at[0], best_sem.at[1], where,
            ).start()

        for inner in range(wide):
            if index == 0:
                pl.when(j != inner)(functools.partial(send_best, inner))
            else:
                send_best(inner)

    tiles = wide // per_tile
    last = len(sources) - 1
    for index in range(last):
        arrive(index)
        new = fetch(index)
        for other in range(index):
            old = fetch(other)
            if index < 3 or other > 0:
                score(new, index, old, other)
            score(old, other, new, index)
        score(new, index, new, index)
    arrive(last)
    new = fetch(last)
    for other in (1, 3, 2, 0):
        if other == 0:
            score(fetch(3), 3, fetch(0), 0)
        score(new, last, fetch(other), other)
        if other != 1:
            answer(other)
    for other in range(last):
        score(fetch(other), other, new, last)
    score(new, last, new, last)
    answer(last)
    best_in[me] = best_out[z * tiles + j // per_tile]

    take_best.wait_recv()
    answers = pltpu.roll(best_in[:, 0, :], (LANES - j * TILE) % LANES, 1)
    spare = best_in[:, 1, :]
    shifted = []
    for p in range(PLANES):
        step = (z + 2 * PLANES - 1 - p) % PLANES
        begin = j % per_tile * PLANES * EXTRA + step * EXTRA
        shifted.append(
            pltpu.roll(spare[p * wide : (p + 1) * wide], (LANES + TILE - begin) % LANES, 1)
        )
    table = jnp.where(lanes < TILE, answers, jnp.concatenate(shifted, axis=0))
    kept = 2 * TILE
    by_row = dot(table[:, :kept], owner_hot.astype(jnp.float32), TN, EXACT)
    out_ref[...] = jnp.sum(jnp.where(lane_hot[:kept], by_row, 0.0), axis=0, keepdims=True)
    take_pools.wait_send()
    for step in range(PLANES - 1):
        remote(meta_out, meta_in.at[step], meta_sem.at[0], meta_sem.at[1], next_one).wait_send()
    take_keys.wait_send()
    take_extra.wait_send()
    sent_rows.wait_send()
    take_best.wait_send()


def pooled_exchange(embeddings, cluster_ids, ranks):
    splits = lax.axis_size("split")
    n = lax.axis_size("loader") * splits
    count, width = embeddings.shape
    big = 1 << (n * count + 1).bit_length()
    wide = n // PLANES
    dma = pltpu.SemaphoreType.DMA

    def held(*shape):
        return pltpu.VMEM(shape, jnp.bfloat16)

    def told(*shape):
        return pltpu.VMEM(shape, jnp.float32)

    return pl.pallas_call(
        functools.partial(pooled_kernel, n, splits, big),
        out_shape=(
            jax.ShapeDtypeStruct((1, count), jnp.float32),
            jax.ShapeDtypeStruct((1, 1), jnp.float32),
        ),
        in_specs=[pl.BlockSpec(memory_space=pl.ANY)] * 3,
        out_specs=(
            pl.BlockSpec(memory_space=pltpu.VMEM), pl.BlockSpec(memory_space=pltpu.SMEM)
        ),
        scratch_shapes=[
            pltpu.VMEM((count, width), embeddings.dtype),
            pltpu.VMEM((1, count), jnp.int32),
            pltpu.VMEM((1, count), jnp.int32),
            *[held(n, TILE, width)] * 2,
            *[held(PLANES * POOL // STRIP, STRIP, width)] * 2,
            *[held(wide, PLANES * EXTRA, width)] * 2,
            told(1, LANES),
            told(PLANES, 1, LANES),
            *[told(n, 1, LANES)] * 2,
            told(PLANES * (wide * PLANES * EXTRA // LANES), 2, LANES),
            told(n, 2, LANES),
            dma((6,)),
            dma,
            dma((PLANES,)),
            *[dma((2,))] * 5,
            pltpu.SemaphoreType.REGULAR,
        ],
        compiler_params=pltpu.CompilerParams(collective_id=0, has_side_effects=True),
    )(embeddings, cluster_ids, ranks)


def two_sizes(embeddings, cluster_ids, ranks):
    n = lax.axis_size("loader") * lax.axis_size("split")
    count = embeddings.shape[0]
    cluster_ids, ranks = cluster_ids.reshape(1, count), ranks.reshape(1, count)
    most = CLUSTERS // n * CAP
    small, over = pooled_exchange(embeddings, cluster_ids, ranks)
    out = lax.cond(
        over[0, 0] > 0.0,
        lambda: exchange(embeddings, cluster_ids, ranks, (TILE, most - TILE), 1)[0],
        lambda: small,
    )
    return out.reshape(count)


def tile_scores(queries, remote):
    return jnp.einsum("kqd,kmd->kqm", queries, remote, preferred_element_type=jnp.float32)


def row_maxima(scores, query_rank, member_rank):
    allowed = (member_rank[:, None, :] >= 0) & (member_rank[:, None, :] < query_rank[:, :, None])
    return jnp.max(jnp.where(allowed, scores, jnp.float32(-1.0)), axis=2)


def small_tiles(embeddings, cluster_ids, ranks):
    loader_count = lax.axis_size("loader")
    split_count = lax.axis_size("split")
    rows_here = embeddings.shape[0]
    width = embeddings.shape[1]
    values = embeddings.astype(jnp.float32)
    unit = (values * lax.rsqrt(jnp.sum(values * values, axis=1, keepdims=True) + epsilon)).astype(
        jnp.bfloat16
    )
    cluster = cluster_ids[:, 0]
    row_index = jnp.arange(rows_here, dtype=jnp.int32)
    same_cluster = cluster[:, None] == cluster[None, :]
    earlier = row_index[None, :] < row_index[:, None]
    position = jnp.sum((same_cluster & earlier).astype(jnp.int32), axis=1)
    slot_count = CLUSTERS * CAP
    device_count = loader_count * split_count
    owner_flat = cluster % device_count
    cluster_slot = cluster // device_count
    owned = CLUSTERS // device_count
    target = (
        (cluster_slot * loader_count + owner_flat // split_count) * split_count
        + owner_flat % split_count
    ) * CAP + position
    send_rows = (
        jnp.zeros((slot_count, width), jnp.bfloat16)
        .at[target]
        .set(unit)
        .reshape(owned, loader_count, split_count, CAP, width)
    )
    send_rank = (
        jnp.full((slot_count,), -1, jnp.int32)
        .at[target]
        .set(ranks)
        .reshape(owned, loader_count, split_count, CAP)
    )

    def swap(block):
        return lax.all_to_all(
            lax.all_to_all(block, "loader", split_axis=1, concat_axis=1, tiled=True),
            "split",
            split_axis=2,
            concat_axis=2,
            tiled=True,
        )

    members = swap(send_rows).reshape(owned, -1, width)
    member_rank = swap(send_rank).reshape(owned, -1)
    best = row_maxima(tile_scores(members, members), member_rank, member_rank)
    returned = swap(best.reshape(owned, loader_count, split_count, CAP))
    return returned.reshape(-1)[target]


def shards(embeddings, cluster_ids, ranks):
    n = lax.axis_size("loader") * lax.axis_size("split")
    fits = n % 4 == 0 and CLUSTERS // n * CAP == 2 * TILE
    fits = fits and n // PLANES % lax.axis_size("split") == 0
    return (two_sizes if fits else small_tiles)(embeddings, cluster_ids, ranks)


def solution(mesh):
    return jax.shard_map(
        shards,
        mesh=mesh,
        in_specs=(
            P(("loader", "split"), None),
            P(("loader", "split"), None),
            P(("loader", "split")),
        ),
        out_specs=P(("loader", "split")),
        check_vma=False,
    )
```
